256 devices in a mesh: groups: 2 (over y), section: 4 (over x), axial: 32 (over z, core).
Axes of the slice: x: 4, y: 2, z: 16, core: 2. Of those that a mesh axis runs over, the one named last changes fastest.
The devices are a block of a 4x16x16 slice.
Arguments:
- pair_in: bfloat16 [8, 256, 256, 128], P('groups', 'axial'), parts along dimension 0, may hold values from -6 to 6
- crop_mask: int32 [8, 256], P('groups'), parts along dimension 0, may hold values 0 or 1
- proj_weights: bfloat16 [4, 5, 128, 128], P('section'), may hold values from -0.5 to 0.5
- out_weights: bfloat16 [4, 128, 128], P('section'), may hold values from -0.5 to 0.5
- up_weights: bfloat16 [4, 128, 512], P('section'), may hold values from -0.5 to 0.5
- down_weights: bfloat16 [4, 512, 128], P('section'), may hold values from -0.25 to 0.25
- norm_gains: bfloat16 [4, 3, 128], P('section'), may hold values from 0.099609375 to 1.8984375
Outputs:
- pair_out: bfloat16 [8, 256, 256, 128], P(('groups', 'section'), 'axial'), parts along dimension 0
The draws below stay inside these ranges and needn't reach their ends.
There are 2 independent parts, one for each index of `groups`. The reference program is written for one: setup_inputs(seed, part) draws one part's arguments, and reference() takes and returns one part's arrays. A program takes and returns all parts, laid end to end along the dimension named above; an argument that names none is the same for every part. Nothing has to cross between parts.
Inputs may be any that keep to these rules, and one draw needn't show every extreme that they name: `crop_mask`: 1 marks a residue inside the crop, 0 a padded one.
All inputs are finite; a program needn't handle non-finite values.
Results may differ from the reference program's by a relative error of at most 0.013.
Values may be sent and summed in bfloat16 or wider, within the bound.
A program may use at most 64 MiB of HBM per device.

```python
import jax
import jax.numpy as jnp
from jax import lax

C = 128
MB = 4
N = 256
BLOCKS = 4
FF = 512


def touch_ends(entries, key, smallest, high):
    extent = entries.shape
    place = [jax.random.randint(jax.random.fold_in(key, axis), (), 0, extent[axis]) for axis in range(len(extent))]
    entries = entries.at[tuple(place)].set(smallest)
    longest = extent.index(max(extent))
    place[longest] = (place[longest] + 1) % extent[longest]
    return entries.at[tuple(place)].set(high)


def shard_levels(key, extent, shards, smallest, largest):
    loudness = 1.0
    for axis_at, blocks in shards:
        steps = jax.random.uniform(jax.random.fold_in(jax.random.fold_in(key, 6), axis_at), (blocks,), jnp.float32, smallest / len(shards), largest / len(shards))
        loudness = loudness * jnp.repeat(jnp.exp(steps), extent[axis_at] // blocks).reshape((-1,) + (1,) * (len(extent) - 1 - axis_at))
    return loudness


def scatter_about(stream_key, dims, scale, reach, split=(), dtype=jnp.bfloat16):
    level = shard_levels(stream_key, dims, split, -0.22, 0.18) if split else 1.0
    drawn = jax.random.normal(stream_key, dims, jnp.float32) * scale * level
    return jnp.minimum(jnp.maximum(drawn, -reach), reach).astype(dtype)


def setup_inputs(seed: int = 0, part: int = 0) -> dict:
    splits = jax.random.split(jax.random.key(seed), 8)
    part_splits = jax.random.split(jax.random.fold_in(splits[7], part), 8)
    pair_in = scatter_about(part_splits[0], (MB, N, N, C), 1.0, 6.0, ((1, 32),))
    crop_mask = touch_ends((jax.random.randint(part_splits[1], (MB, N), 0, 8) < 7).astype(jnp.int32), jax.random.fold_in(part_splits[1], 1), 0, 1)
    proj_weights = scatter_about(splits[2], (BLOCKS, 5, C, C), C ** -0.5, 0.5, ((0, 4),))
    out_weights = scatter_about(splits[3], (BLOCKS, C, C), C ** -0.5, 0.5, ((0, 4),))
    up_weights = scatter_about(splits[4], (BLOCKS, C, FF), C ** -0.5, 0.5, ((0, 4),))
    down_weights = scatter_about(splits[5], (BLOCKS, FF, C), FF ** -0.5, 0.25, ((0, 4),))
    norm_gains = jnp.clip(1.0 + 0.18 * jax.random.normal(splits[6], (BLOCKS, 3, C), jnp.float32), 0.099609375, 1.8984375).astype(jnp.bfloat16)
    return dict(pair_in=pair_in, crop_mask=crop_mask, proj_weights=proj_weights, out_weights=out_weights, up_weights=up_weights, down_weights=down_weights, norm_gains=norm_gains)


epsilon = 1e-05

def normalize(values, axis_dim):
    center = values - lax.optimization_barrier(jnp.mean(values, axis=axis_dim, keepdims=True))
    spread = lax.optimization_barrier(jnp.mean(center * center, axis=axis_dim, keepdims=True))
    return center * lax.rsqrt(spread + epsilon)

def evo_block(current, mask_all, proj_mats, out_mat, up_mat, down_mat, gain_rows):
    channels = current.shape[2]
    gain_vals = gain_rows.astype(jnp.float32)
    pair_f = current.astype(jnp.float32)
    normed = (normalize(pair_f, 2) * gain_vals[0]).astype(jnp.bfloat16)
    linear = jnp.einsum('ijd,edc->ecij', normed.astype(jnp.float32), proj_mats[:4].astype(jnp.float32))
    pair_mask = mask_all[:, None] * mask_all[None, :]
    left_edge = (jax.nn.sigmoid(linear[1]) * linear[0] * pair_mask).astype(jnp.bfloat16)
    right_edge = (jax.nn.sigmoid(linear[3]) * linear[2] * pair_mask).astype(jnp.bfloat16)
    product = jnp.einsum('cik,cjk->cij', left_edge.astype(jnp.float32), right_edge.astype(jnp.float32)).astype(jnp.bfloat16)
    tri_norm = (normalize(product.astype(jnp.float32), 0) * gain_vals[1][:, None, None]).astype(jnp.bfloat16)
    update = jnp.einsum('cij,cd->ijd', tri_norm.astype(jnp.float32), out_mat.astype(jnp.float32))
    gate_values = jax.nn.sigmoid(jnp.einsum('ijd,dc->ijc', normed.astype(jnp.float32), proj_mats[4].astype(jnp.float32)))
    pair_mid = pair_f + gate_values * update
    trans_in = (normalize(pair_mid, 2) * gain_vals[2]).astype(jnp.bfloat16).reshape(-1, channels)
    hidden = jax.nn.relu(jnp.dot(trans_in, up_mat, preferred_element_type=jnp.float32)).astype(jnp.bfloat16)
    pair_new = pair_mid + jnp.dot(hidden, down_mat, preferred_element_type=jnp.float32).reshape(pair_mid.shape)
    return pair_new.astype(jnp.bfloat16)

def reference(pair_in, crop_mask, proj_weights, out_weights, up_weights, down_weights, norm_gains):
    finished = []
    for micro_index in range(MB):
        current = pair_in[micro_index]
        mask_all = crop_mask[micro_index].astype(jnp.float32)
        for layer_index in range(BLOCKS):
            current = evo_block(current, mask_all, proj_weights[layer_index], out_weights[layer_index], up_weights[layer_index], down_weights[layer_index], norm_gains[layer_index])
        finished.append(current)
    return jnp.stack(finished)
```

```python
import functools

import jax
import jax.numpy as jnp
from jax import lax
from jax.experimental import pallas as pl
from jax.experimental.pallas import tpu as pltpu
from jax.sharding import PartitionSpec as P

EPS = 1e-05
MESH = pl.DeviceIdType.MESH
F32 = jnp.float32
BF16 = jnp.bfloat16
LANES = 128
SUB = 8


def sigmoid(v):
    return 0.5 * jnp.tanh(0.5 * v) + 0.5


def norm_rows(v):
    center = v - jnp.mean(v, axis=0, keepdims=True)
    spread = jnp.mean(center * center, axis=0, keepdims=True)
    return center * lax.rsqrt(spread + EPS)


def mm(a, b):
    return jnp.dot(a, b, preferred_element_type=F32)


def kernel(
    S, G, R, C, FF, blocks,
    pair_ref, mask_ref, proj_ref, wout_ref, up_ref, down_ref, gain_ref,
    out_ref,
    XB, ZIN, ZT, NB, GATE, SB, LB, TB, OB, S2L, S2R, S3, RS, PM, ZO, YA, YB,
    WP, WO, WU, WD, GN, WPT, WOT, WUT, WDT, GC,
    in_send, in_recv, out_send, out_recv,
    xb_send, xb_recv, z_send, z_recv,
    ya_send, ya_recv, yb_send, yb_recv, o_send, o_recv,
    w_send, w_recv,
):
    M = S * G
    E = R // S
    CPO = C // M
    x = lax.axis_index("section")
    A = lax.axis_index("axial")
    m = lax.div(A, G)
    t = lax.rem(A, G)
    a = x * G + t

    def wrap(v, n):
        return lax.rem(v + 2 * n, n)

    def member(d):
        return {"section": lax.div(d, G), "axial": m * G + lax.rem(d, G)}

    def along_z(seg):
        return {"section": x, "axial": seg * G + t}

    def along_x(sec):
        return {"section": sec, "axial": A}

    def remote(src, dst, ss, rs, dev):
        return pltpu.make_async_remote_copy(
            src_ref=src, dst_ref=dst, send_sem=ss, recv_sem=rs,
            device_id=dev, device_id_type=MESH,
        )

    barrier = pltpu.get_barrier_semaphore()

    def greet(k, c):
        pl.semaphore_signal(
            barrier, inc=1, device_id=member(lax.rem(a + k, M)), device_id_type=MESH
        )
        return c

    lax.fori_loop(1, M, greet, 0)
    for k in range(1, S):
        pl.semaphore_signal(
            barrier, inc=1, device_id=along_z(wrap(m + k, S)), device_id_type=MESH
        )
    pl.semaphore_wait(barrier, M - 1 + S - 1)

    def xb_copy(k, h):
        dest = wrap(m + k, S)
        return remote(
            pair_ref.at[dest, pl.ds(E * x, E), pl.ds(h * LANES, LANES), :],
            XB.at[m, h],
            xb_send.at[k, h], xb_recv.at[k, h], along_z(dest),
        )

    def xb_local(h):
        return pltpu.make_async_copy(
            pair_ref.at[m, pl.ds(E * x, E), pl.ds(h * LANES, LANES), :],
            XB.at[m, h], xb_recv.at[0, h],
        )

    weights = ((proj_ref, WP), (wout_ref, WO), (up_ref, WU), (down_ref, WD), (gain_ref, GN))

    def w_copy(k, i):
        src, dst = weights[i]
        return remote(
            src.at[0], dst.at[x], w_send.at[k, i], w_recv.at[k, i], along_x(wrap(x + k, S))
        )

    def w_local(i):
        src, dst = weights[i]
        return pltpu.make_async_copy(src.at[0], dst.at[x], w_recv.at[0, i])

    order = (S // 2,) + tuple(k for k in range(1, S) if k != S // 2)
    for h in range(2):
        for k in order:
            xb_copy(k, h).start()
        xb_local(h).start()
    for i in range(len(weights)):
        w_local(i).start()
        for k in range(1, S):
            w_copy(k, i).start()

    q = mask_ref[pl.ds(m, 1), :].astype(F32)
    n_res = q.shape[1]
    lane = lax.broadcasted_iota(jnp.int32, (R, n_res), 1)
    row = lax.broadcasted_iota(jnp.int32, (R, n_res), 0) + a * R
    q_rows = jnp.sum(jnp.where(lane == row, q, 0.0), axis=1, keepdims=True)
    pair_mask = q_rows * q
    for h in range(2):
        PM[h] = pair_mask[:, h * LANES : (h + 1) * LANES]

    for i in range(len(weights)):
        w_local(i).wait()
        for k in range(1, S):
            w_copy(k, i).wait_recv()

    def flip(v):
        return v.astype(F32).T.astype(BF16)

    def flip_weights(l, c):
        for e in range(5):
            WPT[l, e * C : (e + 1) * C, :] = flip(WP[l, e])
        WOT[l] = flip(WO[l])
        for f in range(FF // C):
            WUT[l, f * C : (f + 1) * C, :] = flip(WU[l, :, f * C : (f + 1) * C])
            WDT[l, :, f * C : (f + 1) * C] = flip(WD[l, f * C : (f + 1) * C, :])
        for g in range(3):
            GC[l, g] = jnp.broadcast_to(GN[l, g : g + 1, :], (LANES, C)).T
        return c

    lax.fori_loop(0, blocks, flip_weights, 0)

    def z_copy(k, h):
        sec = wrap(x + k, S)
        return remote(
            XB.at[sec, h], ZIN.at[h, pl.ds(E * x, E)],
            z_send.at[k, h], z_recv.at[k, h], along_x(sec),
        )

    def forward(h):
        for k in order + (0,):
            sec = wrap(x + k, S)
            kz = wrap(m - sec, S)
            pltpu.make_async_copy(XB.at[sec, h], XB.at[sec, h], xb_recv.at[kz, h]).wait()
            if k:
                z_copy(k, h).start()
            else:
                ZIN[h, pl.ds(E * x, E)] = XB[x, h]

    def gather_in(h):
        for k in range(1, S):
            z_copy(k, h).wait_recv()

        def turn(rp, c):
            parts = [ZIN[h, 2 * rp + e].astype(F32).T for e in range(2)]
            ZT[h, rp] = jnp.concatenate(parts, axis=1).astype(BF16)
            return c

        lax.fori_loop(0, R // 2, turn, 0)

    def wide(v):
        return jnp.concatenate([v, v], axis=1)

    def in_copy(h, d):
        return remote(
            SB.at[h, d], LB.at[h, a], in_send.at[h], in_recv.at[h], member(d)
        )

    def in_all(h):
        return remote(
            SB.at[h, pl.ds(0, M - 1)], LB.at[h, pl.ds(0, M - 1)],
            in_send.at[h], in_recv.at[h], member(lax.rem(a + 1, M)),
        )

    def out_copy(h, d):
        return remote(
            TB.at[h, d], OB.at[h, a], out_send.at[h], out_recv.at[h], member(d)
        )

    def out_all(h):
        return remote(
            TB.at[h, pl.ds(0, M - 1)], OB.at[h, pl.ds(0, M - 1)],
            out_send.at[h], out_recv.at[h], member(lax.rem(a + 1, M)),
        )

    def start_all(copy, h):
        def go(k, c):
            copy(h, lax.rem(a + k, M)).start()
            return c

        lax.fori_loop(1, M, go, 0)

    def pre(l, h):
        g0 = wide(GC[l, 0])

        def project(rp, c):
            normed = (norm_rows(ZT[h, rp].astype(F32)) * g0).astype(BF16)
            NB[h, rp] = normed
            lin = mm(WPT[l, 0 : 4 * C, :], normed)
            pm = jnp.concatenate([PM[h, pl.ds(2 * rp, 1), :], PM[h, pl.ds(2 * rp + 1, 1), :]], axis=1)
            left = sigmoid(lin[C : 2 * C]) * lin[0:C] * pm
            right = sigmoid(lin[3 * C : 4 * C]) * lin[2 * C : 3 * C] * pm
            for e in range(2):
                rows = pl.ds(2 * rp + e, C, stride=SUB)
                S2L[rows, :] = left[:, e * LANES : (e + 1) * LANES]
                S2R[rows, :] = right[:, e * LANES : (e + 1) * LANES]
            return c

        lax.fori_loop(0, R // 2, project, 0)

        @pl.when(l > 0)
        def _():
            in_all(h).wait_send()

        SB[h, :, 0] = S2L[...].reshape(M, CPO, SUB, LANES).astype(BF16)
        SB[h, :, 1] = S2R[...].reshape(M, CPO, SUB, LANES).astype(BF16)
        start_all(in_copy, h)
        LB[h, a] = SB[h, a]

        def gates(rp, c):
            GATE[h, rp] = sigmoid(mm(WPT[l, 4 * C : 5 * C, :], NB[h, rp]))
            return c

        lax.fori_loop(0, R // 2, gates, 0)

    def triangle(l):
        for h in range(2):
            in_all(h).wait_recv()

        @pl.when(l > 0)
        def _():
            for h in range(2):
                out_all(h).wait_send()

        def channel(c, carry):
            def side(lr):
                halves = [
                    LB[h, :, lr, c].astype(F32).reshape(M * SUB, LANES).astype(BF16)
                    for h in range(2)
                ]
                return jnp.concatenate(halves, axis=1)

            prod = lax.dot_general(
                side(0), side(1), (((1,), (1,)), ((), ())), preferred_element_type=F32
            )
            for h in range(2):
                TB[h, :, c] = (
                    prod[:, h * LANES : (h + 1) * LANES].reshape(M, SUB, LANES).astype(BF16)
                )
            return carry

        lax.fori_loop(0, CPO, channel, 0)
        for h in range(2):
            start_all(out_copy, h)
        for h in range(2):
            OB[h, a] = TB[h, a]

    def post(l, h):
        out_all(h).wait_recv()
        got = OB[h].astype(F32).reshape(C, SUB, LANES)
        mean = jnp.sum(got, axis=0) * (1.0 / C)
        center = got - mean[None]
        S3[...] = center.reshape(C * SUB, LANES)
        RS[...] = lax.rsqrt(jnp.sum(center * center, axis=0) * (1.0 / C) + EPS)
        g1 = wide(GC[l, 1])
        g2 = wide(GC[l, 2])

        def update(rp, c):
            vals = jnp.concatenate(
                [S3[pl.ds(2 * rp + e, C, stride=SUB), :] for e in range(2)], axis=1
            )
            scale = jnp.concatenate([RS[pl.ds(2 * rp + e, 1), :] for e in range(2)], axis=1)
            tri_norm = (vals * scale * g1).astype(BF16)
            mid = ZT[h, rp].astype(F32) + GATE[h, rp] * mm(WOT[l], tri_norm)
            trans_in = (norm_rows(mid) * g2).astype(BF16)
            hidden = jnp.maximum(mm(WUT[l], trans_in), 0.0).astype(BF16)
            ZT[h, rp] = (mid + mm(WDT[l], hidden)).astype(BF16)
            return c

        lax.fori_loop(0, R // 2, update, 0)

    for h in range(2):
        forward(h)
    for h in range(2):
        gather_in(h)
        pre(0, h)

    def block(l, c):
        triangle(l)
        for h in range(2):
            post(l, h)

            @pl.when(l < blocks - 1)
            def _():
                pre(l + 1, h)

        return c

    lax.fori_loop(0, blocks, block, 0)

    def ya_copy(k, h):
        sec = wrap(x + k, S)
        return remote(
            ZO.at[h, pl.ds(E * sec, E)], YA.at[x, h],
            ya_send.at[k, h], ya_recv.at[k, h], along_x(sec),
        )

    def yb_copy(k, h):
        seg = wrap(m + k, S)
        return remote(
            YA.at[seg, h], YB.at[m, h], yb_send.at[k, h], yb_recv.at[k, h], along_z(seg)
        )

    def o_slice(h):
        return out_ref.at[0, pl.ds(E * x, E), pl.ds(h * LANES, LANES), :]

    def o_copy(k, h):
        sec = wrap(x + k, S)
        return remote(
            YB.at[sec, h], o_slice(h), o_send.at[k, h], o_recv.at[k, h], along_x(sec)
        )

    def o_local(h):
        return pltpu.make_async_copy(YB.at[x, h], o_slice(h), o_recv.at[0, h])

    for h in range(2):
        def turn_back(rp, c, h=h):
            v = ZT[h, rp].astype(F32)
            for e in range(2):
                ZO[h, 2 * rp + e] = v[:, e * LANES : (e + 1) * LANES].T.astype(BF16)
            return c

        lax.fori_loop(0, R // 2, turn_back, 0)
        for k in order:
            ya_copy(k, h).start()
        YA[x, h] = ZO[h, pl.ds(E * x, E)]
    for h in range(2):
        for k in order + (0,):
            seg = wrap(m + k, S)
            kx = wrap(x - seg, S)

            @pl.when(kx != 0)
            def _():
                pltpu.make_async_copy(YA.at[seg, h], YA.at[seg, h], ya_recv.at[kx, h]).wait()

            if k:
                yb_copy(k, h).start()
            else:
                YB[m, h] = YA[m, h]
    for h in range(2):
        for k in order + (0,):
            sec = wrap(x + k, S)
            kz = wrap(m - sec, S)

            @pl.when(kz != 0)
            def _():
                pltpu.make_async_copy(YB.at[sec, h], YB.at[sec, h], yb_recv.at[kz, h]).wait()

            if k:
                o_copy(k, h).start()
            else:
                o_local(h).start()
    for h in range(2):
        in_all(h).wait_send()
        out_all(h).wait_send()
        o_local(h).wait()
        for k in range(1, S):
            xb_copy(k, h).wait_send()
            z_copy(k, h).wait_send()
            ya_copy(k, h).wait_send()
            yb_copy(k, h).wait_send()
            o_copy(k, h).wait_send()
            o_copy(k, h).wait_recv()
    for i in range(len(weights)):
        for k in range(1, S):
            w_copy(k, i).wait_send()


def per_device(pair_in, crop_mask, proj_weights, out_weights, up_weights, down_weights, norm_gains):
    S = lax.axis_size("section")
    G = lax.axis_size("axial") // S
    MB, R, N, C = pair_in.shape
    FF = up_weights.shape[-1]
    M = S * G
    CPO = C // M
    E = R // S
    assert MB == S and R == SUB and N == 2 * LANES and C == LANES and N == R * M
    gains = jnp.pad(norm_gains.astype(F32), ((0, 0), (0, SUB - norm_gains.shape[1]), (0, 0)))
    any_spec = pl.BlockSpec(memory_space=pl.ANY)
    vmem_spec = pl.BlockSpec(memory_space=pltpu.VMEM)
    V = pltpu.VMEM
    dma = pltpu.SemaphoreType.DMA
    return pl.pallas_call(
        functools.partial(kernel, S, G, R, C, FF, S),
        out_shape=jax.ShapeDtypeStruct((1, R, N, C), BF16),
        in_specs=[any_spec, vmem_spec] + [any_spec] * 5,
        out_specs=any_spec,
        scratch_shapes=[
            V((S, 2, E, LANES, C), BF16),
            V((2, R, LANES, C), BF16),
            V((2, R // 2, C, 2 * LANES), BF16),
            V((2, R // 2, C, 2 * LANES), BF16),
            V((2, R // 2, C, 2 * LANES), F32),
            V((2, M, 2, CPO, SUB, LANES), BF16),
            V((2, M, 2, CPO, SUB, LANES), BF16),
            V((2, M, CPO, SUB, LANES), BF16),
            V((2, M, CPO, SUB, LANES), BF16),
            V((C * SUB, LANES), F32),
            V((C * SUB, LANES), F32),
            V((C * SUB, LANES), F32),
            V((SUB, LANES), F32),
            V((2, SUB, LANES), F32),
            V((2, R, LANES, C), BF16),
            V((S, 2, E, LANES, C), BF16),
            V((S, 2, E, LANES, C), BF16),
            V((S, 5, C, C), BF16),
            V((S, C, C), BF16),
            V((S, C, FF), BF16),
            V((S, FF, C), BF16),
            V((S, SUB, C), F32),
            V((S, 5 * C, C), BF16),
            V((S, C, C), BF16),
            V((S, FF, C), BF16),
            V((S, C, FF), BF16),
            V((S, 3, C, LANES), F32),
        ]
        + [dma((2,))] * 4
        + [dma((S, 2))] * 10
        + [dma((S, 5))] * 2,
        compiler_params=pltpu.CompilerParams(
            collective_id=0, has_side_effects=True, vmem_limit_bytes=56 * 1024 * 1024
        ),
    )(pair_in, crop_mask, proj_weights, out_weights, up_weights, down_weights, gains)


def solution(mesh):
    return jax.shard_map(
        per_device,
        mesh=mesh,
        in_specs=(
            P("groups", "axial", None, None),
            P("groups", None),
            P("section", None, None, None),
            P("section", None, None),
            P("section", None, None),
            P("section", None, None),
            P("section", None, None),
        ),
        out_specs=P(("groups", "section"), "axial", None, None),
        check_vma=False,
    )
```

```python
import functools

import jax
import jax.numpy as jnp
from jax import lax
from jax.experimental import pallas as pl
from jax.experimental.pallas import tpu as pltpu
from jax.sharding import PartitionSpec as P

EPS = 1e-05
MESH = pl.DeviceIdType.MESH
F32 = jnp.float32
BF16 = jnp.bfloat16
LANES = 128
SUB = 8


def sigmoid(v):
    return 0.5 * jnp.tanh(0.5 * v) + 0.5


def norm_rows(v):
    center = v - jnp.mean(v, axis=0, keepdims=True)
    spread = jnp.mean(center * center, axis=0, keepdims=True)
    return center * lax.rsqrt(spread + EPS)


def mm(a, b):
    return jnp.dot(a, b, preferred_element_type=F32)


def kernel(
    S, G, R, C, FF, blocks,
    pair_ref, mask_ref, proj_ref, wout_ref, up_ref, down_ref, gain_ref,
    out_ref,
    XB, ZIN, ZT, NB, GATE, SB, LB, TB, OB, S2L, S2R, S3, RS, PM, ZO, YA, YB,
    WP, WO, WU, WD, GN, WPT, WOT, WUT, WDT, GC,
    in_send, in_recv, out_send, out_recv,
    xb_send, xb_recv, z_send, z_recv,
    ya_send, ya_recv, yb_send, yb_recv, o_send, o_recv,
    w_send, w_recv,
):
    M = S * G
    E = R // S
    CPO = C // M
    x = lax.axis_index("section")
    A = lax.axis_index("axial")
    m = lax.div(A, G)
    t = lax.rem(A, G)
    a = x * G + t

    def wrap(v, n):
        return lax.rem(v + 2 * n, n)

    def member(d):
        return {"section": lax.div(d, G), "axial": m * G + lax.rem(d, G)}

    def along_z(seg):
        return {"section": x, "axial": seg * G + t}

    def along_x(sec):
        return {"section": sec, "axial": A}

    def remote(src, dst, ss, rs, dev):
        return pltpu.make_async_remote_copy(
            src_ref=src, dst_ref=dst, send_sem=ss, recv_sem=rs,
            device_id=dev, device_id_type=MESH,
        )

    barrier = pltpu.get_barrier_semaphore()

    def greet(k, c):
        pl.semaphore_signal(
            barrier, inc=1, device_id=member(lax.rem(a + k, M)), device_id_type=MESH
        )
        return c

    lax.fori_loop(1, M, greet, 0)
    for k in range(1, S):
        pl.semaphore_signal(
            barrier, inc=1, device_id=along_z(wrap(m + k, S)), device_id_type=MESH
        )
    pl.semaphore_wait(barrier, M - 1 + S - 1)

    def xb_copy(k, h):
        dest = wrap(m + k, S)
        return remote(
            pair_ref.at[dest, pl.ds(E * x, E), pl.ds(h * LANES, LANES), :],
            XB.at[m, h],
            xb_send.at[k, h], xb_recv.at[k, h], along_z(dest),
        )

    def xb_local(h):
        return pltpu.make_async_copy(
            pair_ref.at[m, pl.ds(E * x, E), pl.ds(h * LANES, LANES), :],
            XB.at[m, h], xb_recv.at[0, h],
        )

    weights = ((proj_ref, WP), (wout_ref, WO), (up_ref, WU), (down_ref, WD), (gain_ref, GN))

    def w_copy(k, i):
        src, dst = weights[i]
        return remote(
            src.at[0], dst.at[x], w_send.at[k, i], w_recv.at[k, i], along_x(wrap(x + k, S))
        )

    def w_local(i):
        src, dst = weights[i]
        return pltpu.make_async_copy(src.at[0], dst.at[x], w_recv.at[0, i])

    def w_send_all(l, which):
        @pl.when(x == l)
        def _():
            for i in which:
                for k in range(1, S):
                    w_copy(k, i).start()

    def w_arrived(l, which):
        k = wrap(x - l, S)
        for i in which:
            dst = weights[i][1]
            pltpu.make_async_copy(dst.at[l], dst.at[l], w_recv.at[k, i]).wait()

    early, late = (0, 4), (1, 2, 3)
    order = (S // 2,) + tuple(k for k in range(1, S) if k != S // 2)
    for h in range(2):
        for k in order:
            xb_copy(k, h).start()
        xb_local(h).start()
    for i in early + late:
        w_local(i).start()
    w_send_all(0, early)

    q = mask_ref[pl.ds(m, 1), :].astype(F32)
    n_res = q.shape[1]
    lane = lax.broadcasted_iota(jnp.int32, (R, n_res), 1)
    row = lax.broadcasted_iota(jnp.int32, (R, n_res), 0) + a * R
    q_rows = jnp.sum(jnp.where(lane == row, q, 0.0), axis=1, keepdims=True)
    pair_mask = q_rows * q
    for h in range(2):
        PM[h] = pair_mask[:, h * LANES : (h + 1) * LANES]

    def flip(v):
        return v.astype(F32).T.astype(BF16)

    def flip_early(l):
        w_arrived(l, early)
        for e in range(5):
            WPT[l, e * C : (e + 1) * C, :] = flip(WP[l, e])
        for g in range(3):
            GC[l, g] = jnp.broadcast_to(GN[l, g : g + 1, :].astype(F32), (LANES, C)).T

    def flip_late(l):
        w_arrived(l, late)
        WOT[l] = flip(WO[l])
        for f in range(FF // C):
            WUT[l, f * C : (f + 1) * C, :] = flip(WU[l, :, f * C : (f + 1) * C])
            WDT[l, :, f * C : (f + 1) * C] = flip(WD[l, f * C : (f + 1) * C, :])

    def z_copy(k, h):
        sec = wrap(x + k, S)
        return remote(
            XB.at[sec, h], ZIN.at[h, pl.ds(E * x, E)],
            z_send.at[k, h], z_recv.at[k, h], along_x(sec),
        )

    def forward(h):
        for k in order + (0,):
            sec = wrap(x + k, S)
            kz = wrap(m - sec, S)
            pltpu.make_async_copy(XB.at[sec, h], XB.at[sec, h], xb_recv.at[kz, h]).wait()
            if k:
                z_copy(k, h).start()
            else:
                ZIN[h, pl.ds(E * x, E)] = XB[x, h]

    def gather_in(h):
        for k in range(1, S):
            z_copy(k, h).wait_recv()

        def turn(rp, c):
            parts = [ZIN[h, 2 * rp + e].astype(F32).T for e in range(2)]
            ZT[h, rp] = jnp.concatenate(parts, axis=1).astype(BF16)
            return c

        lax.fori_loop(0, R // 2, turn, 0)

    def wide(v):
        return jnp.concatenate([v, v], axis=1)

    def in_copy(h, d):
        return remote(
            SB.at[h, d], LB.at[h, a], in_send.at[h], in_recv.at[h], member(d)
        )

    def in_all(h):
        return remote(
            SB.at[h, pl.ds(0, M - 1)], LB.at[h, pl.ds(0, M - 1)],
            in_send.at[h], in_recv.at[h], member(lax.rem(a + 1, M)),
        )

    def out_copy(h, d):
        return remote(
            TB.at[h, d], OB.at[h, a], out_send.at[h], out_recv.at[h], member(d)
        )

    def out_all(h):
        return remote(
            TB.at[h, pl.ds(0, M - 1)], OB.at[h, pl.ds(0, M - 1)],
            out_send.at[h], out_recv.at[h], member(lax.rem(a + 1, M)),
        )

    def start_all(copy, h):
        def go(k, c):
            copy(h, lax.rem(a + k, M)).start()
            return c

        lax.fori_loop(1, M, go, 0)

    def pre(l, h):
        g0 = wide(GC[l, 0])

        def project(rp, c):
            normed = (norm_rows(ZT[h, rp].astype(F32)) * g0).astype(BF16)
            NB[h, rp] = normed
            lin = mm(WPT[l, 0 : 4 * C, :], normed)
            pm = jnp.concatenate([PM[h, pl.ds(2 * rp, 1), :], PM[h, pl.ds(2 * rp + 1, 1), :]], axis=1)
            left = sigmoid(lin[C : 2 * C]) * lin[0:C] * pm
            right = sigmoid(lin[3 * C : 4 * C]) * lin[2 * C : 3 * C] * pm
            for e in range(2):
                rows = pl.ds(2 * rp + e, C, stride=SUB)
                S2L[rows, :] = left[:, e * LANES : (e + 1) * LANES]
                S2R[rows, :] = right[:, e * LANES : (e + 1) * LANES]
            return c

        lax.fori_loop(0, R // 2, project, 0)

        @pl.when(l > 0)
        def _():
            in_all(h).wait_send()

        SB[h, :, 0] = S2L[...].reshape(M, CPO, SUB, LANES).astype(BF16)
        SB[h, :, 1] = S2R[...].reshape(M, CPO, SUB, LANES).astype(BF16)
        start_all(in_copy, h)
        LB[h, a] = SB[h, a]

        def gates(rp, c):
            GATE[h, rp] = sigmoid(mm(WPT[l, 4 * C : 5 * C, :], NB[h, rp]))
            return c

        lax.fori_loop(0, R // 2, gates, 0)

    def triangle(l):
        for h in range(2):
            in_all(h).wait_recv()

        @pl.when(l > 0)
        def _():
            for h in range(2):
                out_all(h).wait_send()

        def channel(c, carry):
            def side(lr):
                halves = [
                    LB[h, :, lr, c].astype(F32).reshape(M * SUB, LANES).astype(BF16)
                    for h in range(2)
                ]
                return jnp.concatenate(halves, axis=1)

            prod = lax.dot_general(
                side(0), side(1), (((1,), (1,)), ((), ())), preferred_element_type=F32
            )
            for h in range(2):
                TB[h, :, c] = (
                    prod[:, h * LANES : (h + 1) * LANES].reshape(M, SUB, LANES).astype(BF16)
                )
            return carry

        lax.fori_loop(0, CPO, channel, 0)
        for h in range(2):
            start_all(out_copy, h)
        for h in range(2):
            OB[h, a] = TB[h, a]

    def post(l, h):
        out_all(h).wait_recv()
        got = OB[h].astype(F32).reshape(C, SUB, LANES)
        mean = jnp.sum(got, axis=0) * (1.0 / C)
        center = got - mean[None]
        S3[...] = center.reshape(C * SUB, LANES)
        RS[...] = lax.rsqrt(jnp.sum(center * center, axis=0) * (1.0 / C) + EPS)
        g1 = wide(GC[l, 1])
        g2 = wide(GC[l, 2])

        def update(rp, c):
            vals = jnp.concatenate(
                [S3[pl.ds(2 * rp + e, C, stride=SUB), :] for e in range(2)], axis=1
            )
            scale = jnp.concatenate([RS[pl.ds(2 * rp + e, 1), :] for e in range(2)], axis=1)
            tri_norm = (vals * scale * g1).astype(BF16)
            mid = ZT[h, rp].astype(F32) + GATE[h, rp] * mm(WOT[l], tri_norm)
            trans_in = (norm_rows(mid) * g2).astype(BF16)
            hidden = jnp.maximum(mm(WUT[l], trans_in), 0.0).astype(BF16)
            ZT[h, rp] = (mid + mm(WDT[l], hidden)).astype(BF16)
            return c

        lax.fori_loop(0, R // 2, update, 0)

    def ya_copy(k, h):
        sec = wrap(x + k, S)
        return remote(
            ZO.at[h, pl.ds(E * sec, E)], YA.at[x, h],
            ya_send.at[k, h], ya_recv.at[k, h], along_x(sec),
        )

    def yb_copy(k, h):
        seg = wrap(m + k, S)
        return remote(
            YA.at[seg, h], YB.at[m, h], yb_send.at[k, h], yb_recv.at[k, h], along_z(seg)
        )

    def o_slice(h):
        return out_ref.at[0, pl.ds(E * x, E), pl.ds(h * LANES, LANES), :]

    def o_copy(k, h):
        sec = wrap(x + k, S)
        return remote(
            YB.at[sec, h], o_slice(h), o_send.at[k, h], o_recv.at[k, h], along_x(sec)
        )

    def o_local(h):
        return pltpu.make_async_copy(YB.at[x, h], o_slice(h), o_recv.at[0, h])

    def spread(h):
        def turn_back(rp, c):
            v = ZT[h, rp].astype(F32)
            for e in range(2):
                ZO[h, 2 * rp + e] = v[:, e * LANES : (e + 1) * LANES].T.astype(BF16)
            return c

        lax.fori_loop(0, R // 2, turn_back, 0)
        for k in order:
            ya_copy(k, h).start()
        YA[x, h] = ZO[h, pl.ds(E * x, E)]

    forward(0)
    flip_early(0)
    gather_in(0)
    pre(0, 0)
    forward(1)
    w_send_all(0, late)
    w_send_all(1, early + late)
    gather_in(1)
    pre(0, 1)

    def block(l, c):
        @pl.when(l < blocks - 2)
        def _():
            w_send_all(l + 2, early + late)

        flip_late(l)

        @pl.when(l < blocks - 1)
        def _():
            flip_early(l + 1)

        triangle(l)
        for h in range(2):
            post(l, h)

            @pl.when(l < blocks - 1)
            def _():
                pre(l + 1, h)

            @pl.when(l == blocks - 1)
            def _():
                spread(h)

        return c

    lax.fori_loop(0, blocks, block, 0)
    for h in range(2):
        for k in order + (0,):
            seg = wrap(m + k, S)
            kx = wrap(x - seg, S)

            @pl.when(kx != 0)
            def _():
                pltpu.make_async_copy(YA.at[seg, h], YA.at[seg, h], ya_recv.at[kx, h]).wait()

            if k:
                yb_copy(k, h).start()
            else:
                YB[m, h] = YA[m, h]
    for h in range(2):
        for k in order + (0,):
            sec = wrap(x + k, S)
            kz = wrap(m - sec, S)

            @pl.when(kz != 0)
            def _():
                pltpu.make_async_copy(YB.at[sec, h], YB.at[sec, h], yb_recv.at[kz, h]).wait()

            if k:
                o_copy(k, h).start()
            else:
                o_local(h).start()
    for h in range(2):
        in_all(h).wait_send()
        out_all(h).wait_send()
        o_local(h).wait()
        for k in range(1, S):
            xb_copy(k, h).wait_send()
            z_copy(k, h).wait_send()
            ya_copy(k, h).wait_send()
            yb_copy(k, h).wait_send()
            o_copy(k, h).wait_send()
            o_copy(k, h).wait_recv()
    for i in range(len(weights)):
        for k in range(1, S):
            w_copy(k, i).wait_send()


def per_device(pair_in, crop_mask, proj_weights, out_weights, up_weights, down_weights, norm_gains):
    S = lax.axis_size("section")
    G = lax.axis_size("axial") // S
    MB, R, N, C = pair_in.shape
    FF = up_weights.shape[-1]
    M = S * G
    CPO = C // M
    E = R // S
    assert MB == S and R == SUB and N == 2 * LANES and C == LANES and N == R * M
    any_spec = pl.BlockSpec(memory_space=pl.ANY)
    vmem_spec = pl.BlockSpec(memory_space=pltpu.VMEM)
    V = pltpu.VMEM
    dma = pltpu.SemaphoreType.DMA
    return pl.pallas_call(
        functools.partial(kernel, S, G, R, C, FF, S),
        out_shape=jax.ShapeDtypeStruct((1, R, N, C), BF16),
        in_specs=[any_spec, vmem_spec] + [any_spec] * 5,
        out_specs=any_spec,
        scratch_shapes=[
            V((S, 2, E, LANES, C), BF16),
            V((2, R, LANES, C), BF16),
            V((2, R // 2, C, 2 * LANES), BF16),
            V((2, R // 2, C, 2 * LANES), BF16),
            V((2, R // 2, C, 2 * LANES), F32),
            V((2, M, 2, CPO, SUB, LANES), BF16),
            V((2, M, 2, CPO, SUB, LANES), BF16),
            V((2, M, CPO, SUB, LANES), BF16),
            V((2, M, CPO, SUB, LANES), BF16),
            V((C * SUB, LANES), F32),
            V((C * SUB, LANES), F32),
            V((C * SUB, LANES), F32),
            V((SUB, LANES), F32),
            V((2, SUB, LANES), F32),
            V((2, R, LANES, C), BF16),
            V((S, 2, E, LANES, C), BF16),
            V((S, 2, E, LANES, C), BF16),
            V((S, 5, C, C), BF16),
            V((S, C, C), BF16),
            V((S, C, FF), BF16),
            V((S, FF, C), BF16),
            V((S, 3, C), BF16),
            V((S, 5 * C, C), BF16),
            V((S, C, C), BF16),
            V((S, FF, C), BF16),
            V((S, C, FF), BF16),
            V((S, 3, C, LANES), F32),
        ]
        + [dma((2,))] * 4
        + [dma((S, 2))] * 10
        + [dma((S, 5))] * 2,
        compiler_params=pltpu.CompilerParams(
            collective_id=0, has_side_effects=True, vmem_limit_bytes=56 * 1024 * 1024
        ),
    )(pair_in, crop_mask, proj_weights, out_weights, up_weights, down_weights, norm_gains)


def solution(mesh):
    return jax.shard_map(
        per_device,
        mesh=mesh,
        in_specs=(
            P("groups", "axial", None, None),
            P("groups", None),
            P("section", None, None, None),
            P("section", None, None),
            P("section", None, None),
            P("section", None, None),
            P("section", None, None),
        ),
        out_specs=P(("groups", "section"), "axial", None, None),
        check_vma=False,
    )
```

```python
import functools

import jax
import jax.numpy as jnp
from jax import lax
from jax.experimental import pallas as pl
from jax.experimental.pallas import tpu as pltpu
from jax.sharding import PartitionSpec as P

EPS = 1e-05
MESH = pl.DeviceIdType.MESH
F32 = jnp.float32
BF16 = jnp.bfloat16
LANES = 128
SUB = 8


def sigmoid(v):
    return 0.5 * jnp.tanh(0.5 * v) + 0.5


def norm_rows(v):
    center = v - jnp.mean(v, axis=0, keepdims=True)
    spread = jnp.mean(center * center, axis=0, keepdims=True)
    return center * lax.rsqrt(spread + EPS)


def mm(a, b):
    return jnp.dot(a, b, preferred_element_type=F32)


def kernel(
    S, G, R, C, FF, blocks,
    pair_ref, mask_ref, proj_ref, wout_ref, up_ref, down_ref, gain_ref,
    out_ref,
    XB, ZIN, ZT, NB, GATE, SB, LL, RR, TB, OB, S2L, S2R, S3, RS, PM, ZO, YA, YB,
    WP, WO, WU, WD, GN, WPT, WOT, WUT, WDT, GC,
    l_send, l_recv, i_send, out_send, out_recv, i_recv,
    xb_send, xb_recv, z_send, z_recv,
    ya_send, ya_recv, yb_send, yb_recv, o_send, o_recv,
    w_send, w_recv, r_send, r_recv,
):
    M = S * G
    GH = G // 2
    MH = M // 2
    E = R // S
    CPO = C // MH
    x = lax.axis_index("section")
    A = lax.axis_index("axial")
    m = lax.div(A, G)
    t = lax.rem(A, G)
    a = x * G + t
    half = lax.div(t, GH)
    mine = x * GH + lax.rem(t, GH)

    def wrap(v, n):
        return lax.rem(v + 2 * n, n)

    def member(d):
        return {"section": lax.div(d, G), "axial": m * G + lax.rem(d, G)}

    def in_half(hf, i):
        return {"section": lax.div(i, GH), "axial": m * G + hf * GH + lax.rem(i, GH)}

    def along_z(seg):
        return {"section": x, "axial": seg * G + t}

    def along_x(sec):
        return {"section": sec, "axial": A}

    def remote(src, dst, ss, rs, dev):
        return pltpu.make_async_remote_copy(
            src_ref=src, dst_ref=dst, send_sem=ss, recv_sem=rs,
            device_id=dev, device_id_type=MESH,
        )

    barrier = pltpu.get_barrier_semaphore()

    def greet(k, c):
        pl.semaphore_signal(
            barrier, inc=1, device_id=member(lax.rem(a + k, M)), device_id_type=MESH
        )
        return c

    lax.fori_loop(1, M, greet, 0)
    for k in range(1, S):
        pl.semaphore_signal(
            barrier, inc=1, device_id=along_z(wrap(m + k, S)), device_id_type=MESH
        )
    pl.semaphore_wait(barrier, M - 1 + S - 1)

    def xb_copy(k, h):
        dest = wrap(m + k, S)
        return remote(
            pair_ref.at[dest, pl.ds(E * x, E), pl.ds(h * LANES, LANES), :],
            XB.at[m, h],
            xb_send.at[k, h], xb_recv.at[k, h], along_z(dest),
        )

    def xb_local(h):
        return pltpu.make_async_copy(
            pair_ref.at[m, pl.ds(E * x, E), pl.ds(h * LANES, LANES), :],
            XB.at[m, h], xb_recv.at[0, h],
        )

    weights = ((proj_ref, WP), (wout_ref, WO), (up_ref, WU), (down_ref, WD), (gain_ref, GN))

    def w_copy(k, i):
        src, dst = weights[i]
        return remote(
            src.at[0], dst.at[x], w_send.at[k, i], w_recv.at[k, i], along_x(wrap(x + k, S))
        )

    def w_local(i):
        src, dst = weights[i]
        return pltpu.make_async_copy(src.at[0], dst.at[x], w_recv.at[0, i])

    core = lax.rem(A, 2)
    sibling = A + 1 - 2 * core

    def w_relay_copy(l, i):
        dst = weights[i][1]
        return remote(
            dst.at[l], dst.at[l], r_send.at[l, i], r_recv.at[l, i],
            {"section": x, "axial": sibling},
        )

    def w_relay(l):
        k = wrap(x - l, S)
        for turn, which in ((0, early), (1, late)):
            @pl.when((x != l) & (core == turn))
            def _():
                for i in which:
                    dst = weights[i][1]
                    pltpu.make_async_copy(dst.at[l], dst.at[l], w_recv.at[k, i]).wait()
                    w_relay_copy(l, i).start()

    def w_arrived(l, which, turn):
        for i in which:
            dst = weights[i][1]

            @pl.when(x == l)
            def _():
                pltpu.make_async_copy(dst.at[l], dst.at[l], w_recv.at[0, i]).wait()

            @pl.when((x != l) & (core != turn))
            def _():
                w_relay_copy(l, i).wait_recv()

    early, late = (0, 4), (1, 2, 3)
    order = (S // 2,) + tuple(k for k in range(1, S) if k != S // 2)
    for h in range(2):
        for k in order:
            xb_copy(k, h).start()
        xb_local(h).start()
    for i in early + late:
        w_local(i).start()
    for turn, which in ((0, early), (1, late)):
        @pl.when(core == turn)
        def _():
            for i in which:
                for k in order:
                    w_copy(k, i).start()

    q = mask_ref[pl.ds(m, 1), :].astype(F32)
    n_res = q.shape[1]
    lane = lax.broadcasted_iota(jnp.int32, (R, n_res), 1)
    row = lax.broadcasted_iota(jnp.int32, (R, n_res), 0) + a * R
    q_rows = jnp.sum(jnp.where(lane == row, q, 0.0), axis=1, keepdims=True)
    pair_mask = q_rows * q
    for h in range(2):
        PM[h] = pair_mask[:, h * LANES : (h + 1) * LANES]

    def flip(v):
        return v.astype(F32).T.astype(BF16)

    def flip_early(l):
        w_arrived(l, early, 0)
        for e in range(5):
            WPT[l, e * C : (e + 1) * C, :] = flip(WP[l, e])
        for g in range(3):
            GC[l, g] = jnp.broadcast_to(GN[l, g : g + 1, :].astype(F32), (LANES, C)).T

    def flip_late(l):
        w_arrived(l, late, 1)
        WOT[l] = flip(WO[l])
        for f in range(FF // C):
            WUT[l, f * C : (f + 1) * C, :] = flip(WU[l, :, f * C : (f + 1) * C])
            WDT[l, :, f * C : (f + 1) * C] = flip(WD[l, f * C : (f + 1) * C, :])

    def z_copy(k, h):
        sec = wrap(x + k, S)
        return remote(
            XB.at[sec, h], ZIN.at[h, pl.ds(E * x, E)],
            z_send.at[k, h], z_recv.at[k, h], along_x(sec),
        )

    def forward(h):
        for k in order + (0,):
            sec = wrap(x + k, S)
            kz = wrap(m - sec, S)
            pltpu.make_async_copy(XB.at[sec, h], XB.at[sec, h], xb_recv.at[kz, h]).wait()
            if k:
                z_copy(k, h).start()
            else:
                ZIN[h, pl.ds(E * x, E)] = XB[x, h]

    def gather_in(h):
        for k in range(1, S):
            z_copy(k, h).wait_recv()

        def turn(rp, c):
            parts = [ZIN[h, 2 * rp + e].astype(F32).T for e in range(2)]
            ZT[h, rp] = jnp.concatenate(parts, axis=1).astype(BF16)
            return c

        lax.fori_loop(0, R // 2, turn, 0)

    def wide(v):
        return jnp.concatenate([v, v], axis=1)

    def left_copy(h, i):
        return remote(
            SB.at[h, i, 0], LL.at[h, mine], l_send.at[h], l_recv.at[h], in_half(half, i)
        )

    def right_copy(par, h, hf, i):
        return remote(
            SB.at[h, i, 1], RR.at[par, h, a], i_send.at[h], i_recv.at[par, h], in_half(hf, i)
        )

    def out_copy(h, i):
        return remote(
            TB.at[h, i], OB.at[h, mine], out_send.at[h], out_recv.at[h], in_half(half, i)
        )

    others = pl.ds(0, MH - 1)
    everyone = pl.ds(0, M - 1)

    def left_all(h):
        return remote(
            LL.at[h, others], LL.at[h, others], l_send.at[h], l_recv.at[h], member(lax.rem(a + 1, M))
        )

    def right_all(par, h):
        return remote(
            RR.at[par, h, everyone], RR.at[par, h, everyone],
            i_send.at[h], i_recv.at[par, h], member(lax.rem(a + 1, M)),
        )

    def out_all(h):
        return remote(
            TB.at[h, others], OB.at[h, others],
            out_send.at[h], out_recv.at[h], member(lax.rem(a + 1, M)),
        )

    def start_in(par, h):
        def go(k, c):
            i = lax.rem(mine + k, MH)
            j = lax.rem(mine + MH - k, MH)
            right_copy(par, h, 1 - half, i).start()

            @pl.when(k > 0)
            def _():
                left_copy(h, j).start()
                right_copy(par, h, half, j).start()

            return c

        lax.fori_loop(0, MH, go, 0)

    def start_out(h):
        def go(k, c):
            out_copy(h, lax.rem(mine + k, MH)).start()
            return c

        lax.fori_loop(1, MH, go, 0)

    def in_sent(h):
        left_all(h).wait_send()
        right_all(0, h).wait_send()

    def pre(l, h):
        g0 = wide(GC[l, 0])

        def project(rp, c):
            normed = (norm_rows(ZT[h, rp].astype(F32)) * g0).astype(BF16)
            NB[h, rp] = normed
            lin = mm(WPT[l, 0 : 4 * C, :], normed)
            pm = jnp.concatenate([PM[h, pl.ds(2 * rp, 1), :], PM[h, pl.ds(2 * rp + 1, 1), :]], axis=1)
            left = sigmoid(lin[C : 2 * C]) * lin[0:C] * pm
            right = sigmoid(lin[3 * C : 4 * C]) * lin[2 * C : 3 * C] * pm
            for e in range(2):
                rows = pl.ds(2 * rp + e, C, stride=SUB)
                S2L[rows, :] = left[:, e * LANES : (e + 1) * LANES]
                S2R[rows, :] = right[:, e * LANES : (e + 1) * LANES]
            return c

        [project(rp, 0) for rp in range(R // 2)]

        @pl.when(l > 0)
        def _():
            in_sent(h)

        par = l % 2
        SB[h, :, 0] = S2L[...].reshape(MH, CPO, SUB, LANES).astype(BF16)
        SB[h, :, 1] = S2R[...].reshape(MH, CPO, SUB, LANES).astype(BF16)
        start_in(par, h)
        LL[h, mine] = SB[h, mine, 0]
        RR[par, h, a] = SB[h, mine, 1]

        def gates(rp, c):
            GATE[h, rp] = sigmoid(mm(WPT[l, 4 * C : 5 * C, :], NB[h, rp]))
            return c

        [gates(rp, 0) for rp in range(R // 2)]

    def triangle(l):
        par = l % 2
        for h in range(2):
            left_all(h).wait_recv()
            right_all(par, h).wait_recv()

        @pl.when(l > 0)
        def _():
            for h in range(2):
                out_all(h).wait_send()

        def channel(c, carry):
            def side(parts):
                flat = [p.astype(F32).reshape(-1, LANES).astype(BF16) for p in parts]
                return jnp.concatenate(flat, axis=1)

            prod = lax.dot_general(
                side([LL[h, :, c] for h in range(2)]),
                side([RR[par, h, :, c] for h in range(2)]),
                (((1,), (1,)), ((), ())),
                preferred_element_type=F32,
            )
            for h in range(2):
                TB[h, :, c] = (
                    prod[:, h * LANES : (h + 1) * LANES].reshape(MH, SUB, LANES).astype(BF16)
                )
            return carry

        lax.fori_loop(0, CPO, channel, 0)
        for h in range(2):
            start_out(h)
        for h in range(2):
            OB[h, mine] = TB[h, mine]

    def post(l, h):
        out_all(h).wait_recv()
        got = OB[h].astype(F32).reshape(C, SUB, LANES)
        mean = jnp.sum(got, axis=0) * (1.0 / C)
        center = got - mean[None]
        S3[...] = center.reshape(C * SUB, LANES)
        RS[...] = lax.rsqrt(jnp.sum(center * center, axis=0) * (1.0 / C) + EPS)
        g1 = wide(GC[l, 1])
        g2 = wide(GC[l, 2])

        def update(rp, c):
            vals = jnp.concatenate(
                [S3[pl.ds(2 * rp + e, C, stride=SUB), :] for e in range(2)], axis=1
            )
            scale = jnp.concatenate([RS[pl.ds(2 * rp + e, 1), :] for e in range(2)], axis=1)
            tri_norm = (vals * scale * g1).astype(BF16)
            mid = ZT[h, rp].astype(F32) + GATE[h, rp] * mm(WOT[l], tri_norm)
            trans_in = (norm_rows(mid) * g2).astype(BF16)
            hidden = jnp.maximum(mm(WUT[l], trans_in), 0.0).astype(BF16)
            ZT[h, rp] = (mid + mm(WDT[l], hidden)).astype(BF16)
            return c

        [update(rp, 0) for rp in range(R // 2)]

    def ya_copy(k, h):
        sec = wrap(x + k, S)
        return remote(
            ZO.at[h, pl.ds(E * sec, E)], YA.at[x, h],
            ya_send.at[k, h], ya_recv.at[k, h], along_x(sec),
        )

    def yb_copy(k, h):
        seg = wrap(m + k, S)
        return remote(
            YA.at[seg, h], YB.at[m, h], yb_send.at[k, h], yb_recv.at[k, h], along_z(seg)
        )

    def o_slice(h):
        return out_ref.at[0, pl.ds(E * x, E), pl.ds(h * LANES, LANES), :]

    def o_copy(k, h):
        sec = wrap(x + k, S)
        return remote(
            YB.at[sec, h], o_slice(h), o_send.at[k, h], o_recv.at[k, h], along_x(sec)
        )

    def o_local(h):
        return pltpu.make_async_copy(YB.at[x, h], o_slice(h), o_recv.at[0, h])

    def spread(h):
        def turn_back(rp, c):
            v = ZT[h, rp].astype(F32)
            for e in range(2):
                ZO[h, 2 * rp + e] = v[:, e * LANES : (e + 1) * LANES].T.astype(BF16)
            return c

        lax.fori_loop(0, R // 2, turn_back, 0)
        for k in order:
            ya_copy(k, h).start()
        YA[x, h] = ZO[h, pl.ds(E * x, E)]

    w_relay(0)
    flip_early(0)
    forward(0)
    for l in range(1, blocks):
        w_relay(l)
    gather_in(0)
    pre(0, 0)
    forward(1)
    gather_in(1)
    pre(0, 1)

    def block(l, c):
        flip_late(l)

        @pl.when(l < blocks - 1)
        def _():
            flip_early(l + 1)

        triangle(l)
        for h in range(2):
            post(l, h)

            @pl.when(l < blocks - 1)
            def _():
                pre(l + 1, h)

            @pl.when(l == blocks - 1)
            def _():
                spread(h)

        return c

    lax.fori_loop(0, blocks, block, 0)
    for h in range(2):
        for k in order + (0,):
            seg = wrap(m + k, S)
            kx = wrap(x - seg, S)

            @pl.when(kx != 0)
            def _():
                pltpu.make_async_copy(YA.at[seg, h], YA.at[seg, h], ya_recv.at[kx, h]).wait()

            if k:
                yb_copy(k, h).start()
            else:
                YB[m, h] = YA[m, h]
    for h in range(2):
        for k in order + (0,):
            sec = wrap(x + k, S)
            kz = wrap(m - sec, S)

            @pl.when(kz != 0)
            def _():
                pltpu.make_async_copy(YB.at[sec, h], YB.at[sec, h], yb_recv.at[kz, h]).wait()

            if k:
                o_copy(k, h).start()
            else:
                o_local(h).start()
    for h in range(2):
        in_sent(h)
        out_all(h).wait_send()
        o_local(h).wait()
        for k in range(1, S):
            xb_copy(k, h).wait_send()
            z_copy(k, h).wait_send()
            ya_copy(k, h).wait_send()
            yb_copy(k, h).wait_send()
            o_copy(k, h).wait_send()
            o_copy(k, h).wait_recv()
    for turn, which in ((0, early), (1, late)):
        @pl.when(core == turn)
        def _():
            for i in which:
                for k in range(1, S):
                    w_copy(k, i).wait_send()
                    w_relay_copy(wrap(x + k, S), i).wait_send()


def per_device(pair_in, crop_mask, proj_weights, out_weights, up_weights, down_weights, norm_gains):
    S = lax.axis_size("section")
    G = lax.axis_size("axial") // S
    MB, R, N, C = pair_in.shape
    FF = up_weights.shape[-1]
    M = S * G
    MH = M // 2
    CPO = C // MH
    E = R // S
    assert G % 2 == 0
    assert MB == S and R == SUB and N == 2 * LANES and C == LANES and N == R * M
    any_spec = pl.BlockSpec(memory_space=pl.ANY)
    vmem_spec = pl.BlockSpec(memory_space=pltpu.VMEM)
    V = pltpu.VMEM
    dma = pltpu.SemaphoreType.DMA
    return pl.pallas_call(
        functools.partial(kernel, S, G, R, C, FF, S),
        out_shape=jax.ShapeDtypeStruct((1, R, N, C), BF16),
        in_specs=[any_spec, vmem_spec] + [any_spec] * 5,
        out_specs=any_spec,
        scratch_shapes=[
            V((S, 2, E, LANES, C), BF16),
            V((2, R, LANES, C), BF16),
            V((2, R // 2, C, 2 * LANES), BF16),
            V((2, R // 2, C, 2 * LANES), BF16),
            V((2, R // 2, C, 2 * LANES), F32),
            V((2, MH, 2, CPO, SUB, LANES), BF16),
            V((2, MH, CPO, SUB, LANES), BF16),
            V((2, 2, M, CPO, SUB, LANES), BF16),
            V((2, MH, CPO, SUB, LANES), BF16),
            V((2, MH, CPO, SUB, LANES), BF16),
            V((C * SUB, LANES), F32),
            V((C * SUB, LANES), F32),
            V((C * SUB, LANES), F32),
            V((SUB, LANES), F32),
            V((2, SUB, LANES), F32),
            V((2, R, LANES, C), BF16),
            V((S, 2, E, LANES, C), BF16),
            V((S, 2, E, LANES, C), BF16),
            V((S, 5, C, C), BF16),
            V((S, C, C), BF16),
            V((S, C, FF), BF16),
            V((S, FF, C), BF16),
            V((S, 3, C), BF16),
            V((S, 5 * C, C), BF16),
            V((S, C, C), BF16),
            V((S, FF, C), BF16),
            V((S, C, FF), BF16),
            V((S, 3, C, LANES), F32),
        ]
        + [dma((2,))] * 5
        + [dma((2, 2))]
        + [dma((S, 2))] * 10
        + [dma((S, 5))] * 4,
        compiler_params=pltpu.CompilerParams(
            collective_id=0, has_side_effects=True, vmem_limit_bytes=56 * 1024 * 1024
        ),
    )(pair_in, crop_mask, proj_weights, out_weights, up_weights, down_weights, norm_gains)


def solution(mesh):
    return jax.shard_map(
        per_device,
        mesh=mesh,
        in_specs=(
            P("groups", "axial", None, None),
            P("groups", None),
            P("section", None, None, None),
            P("section", None, None),
            P("section", None, None),
            P("section", None, None),
            P("section", None, None),
        ),
        out_specs=P(("groups", "section"), "axial", None, None),
        check_vma=False,
    )
```

```python
import functools

import jax
import jax.numpy as jnp
from jax import lax
from jax.experimental import pallas as pl
from jax.experimental.pallas import tpu as pltpu
from jax.sharding import PartitionSpec as P

EPS = 1e-05
MESH = pl.DeviceIdType.MESH
F32 = jnp.float32
BF16 = jnp.bfloat16
LANES = 128
SUB = 8


def sigmoid(v):
    return 0.5 * jnp.tanh(0.5 * v) + 0.5


def norm_rows(v):
    center = v - jnp.mean(v, axis=0, keepdims=True)
    spread = jnp.mean(center * center, axis=0, keepdims=True)
    return center * lax.rsqrt(spread + EPS)


def mm(a, b):
    return jnp.dot(a, b, preferred_element_type=F32)


def kernel(
    S, G, R, C, FF, blocks,
    pair_ref, mask_ref, proj_ref, wout_ref, up_ref, down_ref, gain_ref,
    out_ref,
    ZIN, ZT, NB, GATE, SB, LL, RR, TB, OB, S2L, S2R, S3, RS, PM, ZO, YA,
    WP, WO, WU, WD, GN, WPT, WOT, WUT, WDT, GC,
    l_send, l_recv, i_send, out_send, out_recv, i_recv,
    z_send, z_recv, ya_send, ya_recv, o_send, o_recv,
    w_send, w_recv, r_send, r_recv,
):
    M = S * G
    GH = G // 2
    MH = M // 2
    E = R // S
    CPO = C // MH
    x = lax.axis_index("section")
    A = lax.axis_index("axial")
    m = lax.div(A, G)
    t = lax.rem(A, G)
    a = x * G + t
    half = lax.div(t, GH)
    mine = x * GH + lax.rem(t, GH)

    def wrap(v, n):
        return lax.rem(v + 2 * n, n)

    def member(d):
        return {"section": lax.div(d, G), "axial": m * G + lax.rem(d, G)}

    def in_half(hf, i):
        return {"section": lax.div(i, GH), "axial": m * G + hf * GH + lax.rem(i, GH)}

    def along_x(sec):
        return {"section": sec, "axial": A}

    def remote(src, dst, ss, rs, dev):
        return pltpu.make_async_remote_copy(
            src_ref=src, dst_ref=dst, send_sem=ss, recv_sem=rs,
            device_id=dev, device_id_type=MESH,
        )

    barrier = pltpu.get_barrier_semaphore()

    def greet(k, c):
        pl.semaphore_signal(
            barrier, inc=1, device_id=member(lax.rem(a + k, M)), device_id_type=MESH
        )
        return c

    lax.fori_loop(1, M, greet, 0)
    @pl.when(x != m)
    def _():
        for sec in range(S):
            pl.semaphore_signal(
                barrier, inc=1, device_id={"section": sec, "axial": x * G + t},
                device_id_type=MESH,
            )

    pl.semaphore_wait(barrier, M - 1 + S - 1)

    def home(seg):
        return {"section": m, "axial": seg * G + t}

    def piece(ref, row, h):
        return ref.at[row, pl.ds(E * x, E), pl.ds(h * LANES, LANES), :]

    def z_copy(k, h):
        dest = wrap(m + k, S)
        return remote(
            piece(pair_ref, dest, h), ZIN.at[h, pl.ds(E * x, E)],
            z_send.at[k, h], z_recv.at[x, h], home(dest),
        )

    def z_start(k, h):
        if k:
            z_copy(k, h).start()
        else:
            @pl.when(x != m)
            def _():
                z_copy(0, h).start()

            @pl.when(x == m)
            def _():
                pltpu.make_async_copy(
                    piece(pair_ref, m, h), ZIN.at[h, pl.ds(E * x, E)], z_recv.at[x, h]
                ).start()

    weights = ((proj_ref, WP), (wout_ref, WO), (up_ref, WU), (down_ref, WD), (gain_ref, GN))

    def w_copy(k, i):
        src, dst = weights[i]
        return remote(
            src.at[0], dst.at[x], w_send.at[k, i], w_recv.at[k, i], along_x(wrap(x + k, S))
        )

    def w_local(i):
        src, dst = weights[i]
        return pltpu.make_async_copy(src.at[0], dst.at[x], w_recv.at[0, i])

    core = lax.rem(A, 2)
    sibling = A + 1 - 2 * core

    def w_relay_copy(l, i):
        dst = weights[i][1]
        return remote(
            dst.at[l], dst.at[l], r_send.at[l, i], r_recv.at[l, i],
            {"section": x, "axial": sibling},
        )

    def w_relay(l):
        k = wrap(x - l, S)
        for turn, which in ((0, early), (1, late)):
            @pl.when((x != l) & (core == turn))
            def _():
                for i in which:
                    dst = weights[i][1]
                    pltpu.make_async_copy(dst.at[l], dst.at[l], w_recv.at[k, i]).wait()
                    w_relay_copy(l, i).start()

    def w_arrived(l, which, turn):
        for i in which:
            dst = weights[i][1]

            @pl.when(x == l)
            def _():
                pltpu.make_async_copy(dst.at[l], dst.at[l], w_recv.at[0, i]).wait()

            @pl.when((x != l) & (core != turn))
            def _():
                w_relay_copy(l, i).wait_recv()

    early, late = (0, 4), (1, 2, 3)
    order = (S // 2,) + tuple(k for k in range(1, S) if k != S // 2)
    for h in range(2):
        for k in order + (0,):
            z_start(k, h)
    for i in early + late:
        w_local(i).start()
    for turn, which in ((0, early), (1, late)):
        @pl.when(core == turn)
        def _():
            for i in which:
                for k in order:
                    w_copy(k, i).start()

    q = mask_ref[pl.ds(m, 1), :].astype(F32)
    n_res = q.shape[1]
    lane = lax.broadcasted_iota(jnp.int32, (R, n_res), 1)
    row = lax.broadcasted_iota(jnp.int32, (R, n_res), 0) + a * R
    q_rows = jnp.sum(jnp.where(lane == row, q, 0.0), axis=1, keepdims=True)
    pair_mask = q_rows * q
    for h in range(2):
        PM[h] = pair_mask[:, h * LANES : (h + 1) * LANES]

    def flip(v):
        return v.astype(F32).T.astype(BF16)

    def flip_early(l):
        w_arrived(l, early, 0)
        for e in range(5):
            WPT[l, e * C : (e + 1) * C, :] = flip(WP[l, e])
        for g in range(3):
            GC[l, g] = jnp.broadcast_to(GN[l, g : g + 1, :].astype(F32), (LANES, C)).T

    def flip_late(l):
        w_arrived(l, late, 1)
        WOT[l] = flip(WO[l])
        for f in range(FF // C):
            WUT[l, f * C : (f + 1) * C, :] = flip(WU[l, :, f * C : (f + 1) * C])
            WDT[l, :, f * C : (f + 1) * C] = flip(WD[l, f * C : (f + 1) * C, :])

    def gather_in(h):
        for sec in range(S):
            rows = ZIN.at[h, pl.ds(E * sec, E)]
            pltpu.make_async_copy(rows, rows, z_recv.at[sec, h]).wait()

        def turn(rp, c):
            parts = [ZIN[h, 2 * rp + e].astype(F32).T for e in range(2)]
            ZT[h, rp] = jnp.concatenate(parts, axis=1).astype(BF16)
            return c

        lax.fori_loop(0, R // 2, turn, 0)

    def wide(v):
        return jnp.concatenate([v, v], axis=1)

    def left_copy(par, h, i):
        return remote(
            SB.at[h, i, 0], LL.at[par, h, mine], l_send.at[h], l_recv.at[h], in_half(half, i)
        )

    def right_copy(par, h, hf, i):
        return remote(
            SB.at[h, i, 1], RR.at[par, h, a], i_send.at[h], i_recv.at[par, h], in_half(hf, i)
        )

    def out_copy(h, i):
        return remote(
            TB.at[h, i], OB.at[h, mine], out_send.at[h], out_recv.at[h], in_half(half, i)
        )

    others = pl.ds(0, MH - 1)
    everyone = pl.ds(0, M - 1)

    def left_all(h):
        return remote(
            LL.at[0, h, others], LL.at[0, h, others], l_send.at[h], l_recv.at[h], member(lax.rem(a + 1, M))
        )

    def right_all(par, h):
        return remote(
            RR.at[par, h, everyone], RR.at[par, h, everyone],
            i_send.at[h], i_recv.at[par, h], member(lax.rem(a + 1, M)),
        )

    def out_all(h):
        return remote(
            TB.at[h, others], OB.at[h, others],
            out_send.at[h], out_recv.at[h], member(lax.rem(a + 1, M)),
        )

    def start_in(par, h):
        def go(k, c):
            i = lax.rem(mine + k, MH)
            j = lax.rem(mine + MH - k, MH)
            right_copy(par, h, 1 - half, i).start()

            @pl.when(k > 0)
            def _():
                left_copy(par, h, j).start()
                right_copy(par, h, half, j).start()

            return c

        lax.fori_loop(0, MH, go, 0)

    def start_out(h):
        def go(k, c):
            out_copy(h, lax.rem(mine + k, MH)).start()
            return c

        lax.fori_loop(1, MH, go, 0)

    def in_sent(h):
        left_all(h).wait_send()
        right_all(0, h).wait_send()

    def pre(l, h):
        g0 = wide(GC[l, 0])

        def project(rp, c):
            normed = (norm_rows(ZT[h, rp].astype(F32)) * g0).astype(BF16)
            NB[h, rp] = normed
            lin = mm(WPT[l, 0 : 4 * C, :], normed)
            pm = jnp.concatenate([PM[h, pl.ds(2 * rp, 1), :], PM[h, pl.ds(2 * rp + 1, 1), :]], axis=1)
            left = sigmoid(lin[C : 2 * C]) * lin[0:C] * pm
            right = sigmoid(lin[3 * C : 4 * C]) * lin[2 * C : 3 * C] * pm
            for e in range(2):
                rows = pl.ds(2 * rp + e, C, stride=SUB)
                S2L[rows, :] = left[:, e * LANES : (e + 1) * LANES]
                S2R[rows, :] = right[:, e * LANES : (e + 1) * LANES]
            return c

        [project(rp, 0) for rp in range(R // 2)]

        @pl.when(l > 0)
        def _():
            in_sent(h)

        par = l % 2
        SB[h, :, 0] = S2L[...].reshape(MH, CPO, SUB, LANES).astype(BF16)
        SB[h, :, 1] = S2R[...].reshape(MH, CPO, SUB, LANES).astype(BF16)
        start_in(par, h)
        LL[par, h, mine] = SB[h, mine, 0]
        RR[par, h, a] = SB[h, mine, 1]

        def gates(rp, c):
            GATE[h, rp] = sigmoid(mm(WPT[l, 4 * C : 5 * C, :], NB[h, rp]))
            return c

        [gates(rp, 0) for rp in range(R // 2)]

    def triangle(l):
        par = l % 2
        for h in range(2):
            left_all(h).wait_recv()
            right_all(par, h).wait_recv()

        @pl.when(l > 0)
        def _():
            for h in range(2):
                out_all(h).wait_send()

        def side(parts):
            flat = [p.astype(F32).reshape(-1, LANES).astype(BF16) for p in parts]
            return jnp.concatenate(flat, axis=1)

        for h in range(2):
            def channel(c, carry):
                prod = lax.dot_general(
                    side([LL[par, e, :, c] for e in range(2)]),
                    side([RR[par, e, h * MH : (h + 1) * MH, c] for e in range(2)]),
                    (((1,), (1,)), ((), ())),
                    preferred_element_type=F32,
                )
                TB[h, :, c] = prod.reshape(MH, SUB, LANES).astype(BF16)
                return carry

            lax.fori_loop(0, CPO, channel, 0, unroll=2)
            start_out(h)
            OB[h, mine] = TB[h, mine]

    def post(l, h):
        out_all(h).wait_recv()
        got = OB[h].astype(F32).reshape(C, SUB, LANES)
        mean = jnp.sum(got, axis=0) * (1.0 / C)
        center = got - mean[None]
        S3[...] = center.reshape(C * SUB, LANES)
        RS[...] = lax.rsqrt(jnp.sum(center * center, axis=0) * (1.0 / C) + EPS)
        g1 = wide(GC[l, 1])
        g2 = wide(GC[l, 2])

        def update(rp, c):
            vals = jnp.concatenate(
                [S3[pl.ds(2 * rp + e, C, stride=SUB), :] for e in range(2)], axis=1
            )
            scale = jnp.concatenate([RS[pl.ds(2 * rp + e, 1), :] for e in range(2)], axis=1)
            tri_norm = (vals * scale * g1).astype(BF16)
            mid = ZT[h, rp].astype(F32) + GATE[h, rp] * mm(WOT[l], tri_norm)
            trans_in = (norm_rows(mid) * g2).astype(BF16)
            hidden = jnp.maximum(mm(WUT[l], trans_in), 0.0).astype(BF16)
            ZT[h, rp] = (mid + mm(WDT[l], hidden)).astype(BF16)
            return c

        [update(rp, 0) for rp in range(R // 2)]

    def ya_copy(k, h):
        sec = wrap(x + k, S)
        return remote(
            ZO.at[h, pl.ds(E * sec, E)], YA.at[x, h],
            ya_send.at[k, h], ya_recv.at[k, h], along_x(sec),
        )

    def o_copy(k, h):
        seg = wrap(m + k, S)
        return remote(
            YA.at[seg, h], piece(out_ref, 0, h), o_send.at[k, h], o_recv.at[x, h], home(seg)
        )

    def spread(h):
        def turn_back(rp, c):
            v = ZT[h, rp].astype(F32)
            for e in range(2):
                ZO[h, 2 * rp + e] = v[:, e * LANES : (e + 1) * LANES].T.astype(BF16)
            return c

        lax.fori_loop(0, R // 2, turn_back, 0)
        for k in order:
            ya_copy(k, h).start()
        YA[x, h] = ZO[h, pl.ds(E * x, E)]

    w_relay(0)
    flip_early(0)
    gather_in(0)
    pre(0, 0)
    for l in range(1, blocks):
        w_relay(l)
    gather_in(1)
    pre(0, 1)

    def block(l, c):
        flip_late(l)

        @pl.when(l < blocks - 1)
        def _():
            flip_early(l + 1)

        triangle(l)
        for h in range(2):
            post(l, h)

            @pl.when(l < blocks - 1)
            def _():
                pre(l + 1, h)

            @pl.when(l == blocks - 1)
            def _():
                spread(h)

        return c

    lax.fori_loop(0, blocks, block, 0)
    for h in range(2):
        for k in order + (0,):
            seg = wrap(m + k, S)
            kx = wrap(x - seg, S)

            @pl.when(kx != 0)
            def _():
                pltpu.make_async_copy(YA.at[seg, h], YA.at[seg, h], ya_recv.at[kx, h]).wait()

            if k:
                o_copy(k, h).start()
            else:
                @pl.when(x != m)
                def _():
                    o_copy(0, h).start()

                @pl.when(x == m)
                def _():
                    pltpu.make_async_copy(
                        YA.at[m, h], piece(out_ref, 0, h), o_recv.at[x, h]
                    ).start()

    for h in range(2):
        in_sent(h)
        out_all(h).wait_send()
        for sec in range(S):
            rows = out_ref.at[0, pl.ds(E * sec, E), pl.ds(h * LANES, LANES), :]
            pltpu.make_async_copy(rows, rows, o_recv.at[sec, h]).wait()
        for k in range(1, S):
            z_copy(k, h).wait_send()
            ya_copy(k, h).wait_send()
            o_copy(k, h).wait_send()

        @pl.when(x != m)
        def _():
            z_copy(0, h).wait_send()
            o_copy(0, h).wait_send()

    for turn, which in ((0, early), (1, late)):
        @pl.when(core == turn)
        def _():
            for i in which:
                for k in range(1, S):
                    w_copy(k, i).wait_send()
                    w_relay_copy(wrap(x + k, S), i).wait_send()


def per_device(pair_in, crop_mask, proj_weights, out_weights, up_weights, down_weights, norm_gains):
    S = lax.axis_size("section")
    G = lax.axis_size("axial") // S
    MB, R, N, C = pair_in.shape
    FF = up_weights.shape[-1]
    M = S * G
    MH = M // 2
    CPO = C // MH
    E = R // S
    assert G % 2 == 0
    assert MB == S and R == SUB and N == 2 * LANES and C == LANES and N == R * M
    any_spec = pl.BlockSpec(memory_space=pl.ANY)
    vmem_spec = pl.BlockSpec(memory_space=pltpu.VMEM)
    V = pltpu.VMEM
    dma = pltpu.SemaphoreType.DMA
    return pl.pallas_call(
        functools.partial(kernel, S, G, R, C, FF, S),
        out_shape=jax.ShapeDtypeStruct((1, R, N, C), BF16),
        in_specs=[any_spec, vmem_spec] + [any_spec] * 5,
        out_specs=any_spec,
        scratch_shapes=[
            V((2, R, LANES, C), BF16),
            V((2, R // 2, C, 2 * LANES), BF16),
            V((2, R // 2, C, 2 * LANES), BF16),
            V((2, R // 2, C, 2 * LANES), F32),
            V((2, MH, 2, CPO, SUB, LANES), BF16),
            V((2, 2, MH, CPO, SUB, LANES), BF16),
            V((2, 2, M, CPO, SUB, LANES), BF16),
            V((2, MH, CPO, SUB, LANES), BF16),
            V((2, MH, CPO, SUB, LANES), BF16),
            V((C * SUB, LANES), F32),
            V((C * SUB, LANES), F32),
            V((C * SUB, LANES), F32),
            V((SUB, LANES), F32),
            V((2, SUB, LANES), F32),
            V((2, R, LANES, C), BF16),
            V((S, 2, E, LANES, C), BF16),
            V((S, 5, C, C), BF16),
            V((S, C, C), BF16),
            V((S, C, FF), BF16),
            V((S, FF, C), BF16),
            V((S, 3, C), BF16),
            V((S, 5 * C, C), BF16),
            V((S, C, C), BF16),
            V((S, FF, C), BF16),
            V((S, C, FF), BF16),
            V((S, 3, C, LANES), F32),
        ]
        + [dma((2,))] * 5
        + [dma((2, 2))]
        + [dma((S, 2))] * 6
        + [dma((S, 5))] * 4,
        compiler_params=pltpu.CompilerParams(
            collective_id=0, has_side_effects=True, vmem_limit_bytes=56 * 1024 * 1024
        ),
    )(pair_in, crop_mask, proj_weights, out_weights, up_weights, down_weights, norm_gains)


def solution(mesh):
    return jax.shard_map(
        per_device,
        mesh=mesh,
        in_specs=(
            P("groups", "axial", None, None),
            P("groups", None),
            P("section", None, None, None),
            P("section", None, None),
            P("section", None, None),
            P("section", None, None),
            P("section", None, None),
        ),
        out_specs=P(("groups", "section"), "axial", None, None),
        check_vma=False,
    )
```

```python
import functools

import jax
import jax.numpy as jnp
from jax import lax
from jax.experimental import pallas as pl
from jax.experimental.pallas import tpu as pltpu
from jax.sharding import PartitionSpec as P

EPS = 1e-05
MESH = pl.DeviceIdType.MESH
F32 = jnp.float32
BF16 = jnp.bfloat16
LANES = 128
SUB = 8


def sigmoid(v):
    return 0.5 * jnp.tanh(0.5 * v) + 0.5


def norm_rows(v):
    center = v - jnp.mean(v, axis=0, keepdims=True)
    spread = jnp.mean(center * center, axis=0, keepdims=True)
    return center * lax.rsqrt(spread + EPS)


def mm(a, b):
    return jnp.dot(a, b, preferred_element_type=F32)


def kernel(
    S, G, R, C, FF, blocks,
    pair_ref, mask_ref, proj_ref, wout_ref, up_ref, down_ref, gain_ref,
    out_ref,
    ZIN, ZT, NB, GATE, SB, LL, RR, PART, TB, OB, S2L, S2R, S3, RS, PM, ZO, YA,
    WP, WO, WU, WD, GN, WPT, WOT, WUT, WDT, GC,
    l_send, l_recv, i_send, out_send, out_recv, i_recv,
    z_send, z_recv, ya_send, ya_recv, o_send, o_recv,
    w_send, w_recv, r_send, r_recv,
):
    M = S * G
    GH = G // 2
    MH = M // 2
    E = R // S
    CPO = C // MH
    x = lax.axis_index("section")
    A = lax.axis_index("axial")
    m = lax.div(A, G)
    t = lax.rem(A, G)
    a = x * G + t
    half = lax.div(t, GH)
    mine = x * GH + lax.rem(t, GH)

    def wrap(v, n):
        return lax.rem(v + 2 * n, n)

    def member(d):
        return {"section": lax.div(d, G), "axial": m * G + lax.rem(d, G)}

    def in_half(hf, i):
        return {"section": lax.div(i, GH), "axial": m * G + hf * GH + lax.rem(i, GH)}

    def along_x(sec):
        return {"section": sec, "axial": A}

    def remote(src, dst, ss, rs, dev):
        return pltpu.make_async_remote_copy(
            src_ref=src, dst_ref=dst, send_sem=ss, recv_sem=rs,
            device_id=dev, device_id_type=MESH,
        )

    barrier = pltpu.get_barrier_semaphore()

    def greet(k, c):
        pl.semaphore_signal(
            barrier, inc=1, device_id=member(lax.rem(a + k, M)), device_id_type=MESH
        )
        return c

    @pl.when(x != m)
    def _():
        for sec in range(S):
            pl.semaphore_signal(
                barrier, inc=1, device_id={"section": sec, "axial": x * G + t},
                device_id_type=MESH,
            )

    lax.fori_loop(1, M, greet, 0)
    pl.semaphore_wait(barrier, M - 1 + S - 1)

    def home(seg):
        return {"section": m, "axial": seg * G + t}

    def piece(ref, row, h):
        return ref.at[row, pl.ds(E * x, E), pl.ds(h * LANES, LANES), :]

    def z_copy(k, h):
        dest = wrap(m + k, S)
        return remote(
            piece(pair_ref, dest, h), ZIN.at[h, pl.ds(E * x, E)],
            z_send.at[k, h], z_recv.at[x, h], home(dest),
        )

    def z_start(k, h):
        if k:
            z_copy(k, h).start()
        else:
            @pl.when(x != m)
            def _():
                z_copy(0, h).start()

            @pl.when(x == m)
            def _():
                pltpu.make_async_copy(
                    piece(pair_ref, m, h), ZIN.at[h, pl.ds(E * x, E)], z_recv.at[x, h]
                ).start()

    weights = ((proj_ref, WP), (wout_ref, WO), (up_ref, WU), (down_ref, WD), (gain_ref, GN))

    def w_copy(k, i):
        src, dst = weights[i]
        return remote(
            src.at[0], dst.at[x], w_send.at[k, i], w_recv.at[k, i], along_x(wrap(x + k, S))
        )

    def w_local(i):
        src, dst = weights[i]
        return pltpu.make_async_copy(src.at[0], dst.at[x], w_recv.at[0, i])

    core = lax.rem(A, 2)
    sibling = A + 1 - 2 * core

    def w_relay_copy(l, i):
        dst = weights[i][1]
        return remote(
            dst.at[l], dst.at[l], r_send.at[l, i], r_recv.at[l, i],
            {"section": x, "axial": sibling},
        )

    def w_relay(l):
        k = wrap(x - l, S)
        for turn, which in ((0, early), (1, late)):
            @pl.when((x != l) & (core == turn))
            def _():
                for i in which:
                    dst = weights[i][1]
                    pltpu.make_async_copy(dst.at[l], dst.at[l], w_recv.at[k, i]).wait()
                    w_relay_copy(l, i).start()

    def w_arrived(l, which, turn):
        for i in which:
            dst = weights[i][1]

            @pl.when(x == l)
            def _():
                pltpu.make_async_copy(dst.at[l], dst.at[l], w_recv.at[0, i]).wait()

            @pl.when((x != l) & (core != turn))
            def _():
                w_relay_copy(l, i).wait_recv()

    early, late = (0, 4), (1, 2, 3)
    order = (S // 2,) + tuple(k for k in range(1, S) if k != S // 2)
    for h in range(2):
        for k in order + (0,):
            z_start(k, h)
    for i in early + late:
        w_local(i).start()
    for turn, which in ((0, early), (1, late)):
        @pl.when(core == turn)
        def _():
            for i in which:
                for k in order:
                    w_copy(k, i).start()

    q = mask_ref[pl.ds(m, 1), :].astype(F32)
    n_res = q.shape[1]
    lane = lax.broadcasted_iota(jnp.int32, (R, n_res), 1)
    row = lax.broadcasted_iota(jnp.int32, (R, n_res), 0) + a * R
    q_rows = jnp.sum(jnp.where(lane == row, q, 0.0), axis=1, keepdims=True)
    pair_mask = q_rows * q
    for h in range(2):
        PM[h] = pair_mask[:, h * LANES : (h + 1) * LANES]

    def flip(v):
        return v.astype(F32).T.astype(BF16)

    def flip_early(l):
        w_arrived(l, early, 0)
        for e in range(5):
            WPT[l, e * C : (e + 1) * C, :] = flip(WP[l, e])
        for g in range(3):
            GC[l, g] = jnp.broadcast_to(GN[l, g : g + 1, :].astype(F32), (LANES, C)).T

    def flip_late(l):
        w_arrived(l, late, 1)
        WOT[l] = flip(WO[l])
        for f in range(FF // C):
            WUT[l, f * C : (f + 1) * C, :] = flip(WU[l, :, f * C : (f + 1) * C])
            WDT[l, :, f * C : (f + 1) * C] = flip(WD[l, f * C : (f + 1) * C, :])

    def gather_in(h):
        for sec in range(S):
            rows = ZIN.at[h, pl.ds(E * sec, E)]
            pltpu.make_async_copy(rows, rows, z_recv.at[sec, h]).wait()

        def turn(rp, c):
            parts = [ZIN[h, 2 * rp + e].astype(F32).T for e in range(2)]
            ZT[h, rp] = jnp.concatenate(parts, axis=1).astype(BF16)
            return c

        lax.fori_loop(0, R // 2, turn, 0)

    def wide(v):
        return jnp.concatenate([v, v], axis=1)

    def left_copy(par, h, i):
        return remote(
            SB.at[h, i, 0], LL.at[par, h, mine], l_send.at[h], l_recv.at[h], in_half(half, i)
        )

    def right_copy(par, h, hf, i):
        return remote(
            SB.at[h, i, 1], RR.at[par, h, a], i_send.at[h], i_recv.at[par, h], in_half(hf, i)
        )

    def out_copy(h, i):
        return remote(
            TB.at[h, i], OB.at[h, mine], out_send.at[h], out_recv.at[h], in_half(half, i)
        )

    others = pl.ds(0, MH - 1)
    everyone = pl.ds(0, M - 1)

    def left_all(h):
        return remote(
            LL.at[0, h, others], LL.at[0, h, others], l_send.at[h], l_recv.at[h], member(lax.rem(a + 1, M))
        )

    def right_all(par, h):
        return remote(
            RR.at[par, h, everyone], RR.at[par, h, everyone],
            i_send.at[h], i_recv.at[par, h], member(lax.rem(a + 1, M)),
        )

    def out_all(h):
        return remote(
            TB.at[h, others], OB.at[h, others],
            out_send.at[h], out_recv.at[h], member(lax.rem(a + 1, M)),
        )

    def start_in(par, h):
        def go(k, c):
            i = lax.rem(mine + k, MH)
            j = lax.rem(mine + MH - k, MH)
            right_copy(par, h, 1 - half, i).start()

            @pl.when(k > 0)
            def _():
                left_copy(par, h, j).start()
                right_copy(par, h, half, j).start()

            return c

        lax.fori_loop(0, MH, go, 0)

    def start_out(h):
        def go(k, c):
            out_copy(h, lax.rem(mine + k, MH)).start()
            return c

        lax.fori_loop(1, MH, go, 0)

    def in_sent(h):
        left_all(h).wait_send()
        right_all(0, h).wait_send()

    def pre(l, h):
        g0 = wide(GC[l, 0])

        def project(rp, c):
            normed = (norm_rows(ZT[h, rp].astype(F32)) * g0).astype(BF16)
            NB[h, rp] = normed
            lin = mm(WPT[l, 0 : 4 * C, :], normed)
            pm = jnp.concatenate([PM[h, pl.ds(2 * rp, 1), :], PM[h, pl.ds(2 * rp + 1, 1), :]], axis=1)
            left = sigmoid(lin[C : 2 * C]) * lin[0:C] * pm
            right = sigmoid(lin[3 * C : 4 * C]) * lin[2 * C : 3 * C] * pm
            for e in range(2):
                rows = pl.ds(2 * rp + e, C, stride=SUB)
                S2L[rows, :] = left[:, e * LANES : (e + 1) * LANES]
                S2R[rows, :] = right[:, e * LANES : (e + 1) * LANES]
            return c

        [project(rp, 0) for rp in range(R // 2)]

        @pl.when(l > 0)
        def _():
            in_sent(h)

        par = l % 2
        SB[h, :, 0] = S2L[...].reshape(MH, CPO, SUB, LANES).astype(BF16)
        SB[h, :, 1] = S2R[...].reshape(MH, CPO, SUB, LANES).astype(BF16)
        start_in(par, h)
        LL[par, h, mine] = SB[h, mine, 0]
        RR[par, h, a] = SB[h, mine, 1]

        def gates(rp, c):
            GATE[h, rp] = sigmoid(mm(WPT[l, 4 * C : 5 * C, :], NB[h, rp]))
            return c

        [gates(rp, 0) for rp in range(R // 2)]

    def triangle(l):
        par = l % 2

        def flat(v):
            return v.astype(F32).reshape(-1, LANES).astype(BF16)

        def outer(p, q):
            return lax.dot_general(
                flat(p), flat(q), (((1,), (1,)), ((), ())), preferred_element_type=F32
            )

        def arrived(e):
            left_all(e).wait_recv()
            right_all(par, e).wait_recv()

        def first(c, carry):
            PART[c] = outer(LL[par, 0, :, c], RR[par, 0, :, c])
            return carry

        arrived(0)
        lax.fori_loop(0, CPO, first, 0, unroll=2)

        @pl.when(l > 0)
        def _():
            for h in range(2):
                out_all(h).wait_send()

        arrived(1)
        for h in range(2):
            def channel(c, carry):
                prod = PART[c, :, h * LANES : (h + 1) * LANES] + outer(
                    LL[par, 1, :, c], RR[par, 1, h * MH : (h + 1) * MH, c]
                )
                TB[h, :, c] = prod.reshape(MH, SUB, LANES).astype(BF16)
                return carry

            lax.fori_loop(0, CPO, channel, 0, unroll=True)
            start_out(h)
            OB[h, mine] = TB[h, mine]

    def post(l, h):
        out_all(h).wait_recv()
        got = OB[h].astype(F32).reshape(C, SUB, LANES)
        mean = jnp.sum(got, axis=0) * (1.0 / C)
        center = got - mean[None]
        S3[...] = center.reshape(C * SUB, LANES)
        RS[...] = lax.rsqrt(jnp.sum(center * center, axis=0) * (1.0 / C) + EPS)
        g1 = wide(GC[l, 1])
        g2 = wide(GC[l, 2])

        def update(rp, c):
            vals = jnp.concatenate(
                [S3[pl.ds(2 * rp + e, C, stride=SUB), :] for e in range(2)], axis=1
            )
            scale = jnp.concatenate([RS[pl.ds(2 * rp + e, 1), :] for e in range(2)], axis=1)
            tri_norm = (vals * scale * g1).astype(BF16)
            mid = ZT[h, rp].astype(F32) + GATE[h, rp] * mm(WOT[l], tri_norm)
            trans_in = (norm_rows(mid) * g2).astype(BF16)
            hidden = jnp.maximum(mm(WUT[l], trans_in), 0.0).astype(BF16)
            ZT[h, rp] = (mid + mm(WDT[l], hidden)).astype(BF16)
            return c

        [update(rp, 0) for rp in range(R // 2)]

    def ya_copy(k, h):
        sec = wrap(x + k, S)
        return remote(
            ZO.at[h, pl.ds(E * sec, E)], YA.at[x, h],
            ya_send.at[k, h], ya_recv.at[k, h], along_x(sec),
        )

    def o_copy(k, h):
        seg = wrap(m + k, S)
        return remote(
            YA.at[seg, h], piece(out_ref, 0, h), o_send.at[k, h], o_recv.at[x, h], home(seg)
        )

    def spread(h):
        def turn_back(rp, c):
            v = ZT[h, rp].astype(F32)
            for e in range(2):
                ZO[h, 2 * rp + e] = v[:, e * LANES : (e + 1) * LANES].T.astype(BF16)
            return c

        lax.fori_loop(0, R // 2, turn_back, 0)
        for k in order:
            ya_copy(k, h).start()
        YA[x, h] = ZO[h, pl.ds(E * x, E)]

    w_relay(0)
    flip_early(0)
    gather_in(0)
    pre(0, 0)
    for l in range(1, blocks):
        w_relay(l)
    gather_in(1)
    pre(0, 1)

    def block(l, c):
        flip_late(l)

        @pl.when(l < blocks - 1)
        def _():
            flip_early(l + 1)

        triangle(l)
        for h in range(2):
            post(l, h)

            @pl.when(l < blocks - 1)
            def _():
                pre(l + 1, h)

            @pl.when(l == blocks - 1)
            def _():
                spread(h)

        return c

    lax.fori_loop(0, blocks, block, 0)
    for h in range(2):
        for k in order + (0,):
            seg = wrap(m + k, S)
            kx = wrap(x - seg, S)

            @pl.when(kx != 0)
            def _():
                pltpu.make_async_copy(YA.at[seg, h], YA.at[seg, h], ya_recv.at[kx, h]).wait()

            if k:
                o_copy(k, h).start()
            else:
                @pl.when(x != m)
                def _():
                    o_copy(0, h).start()

                @pl.when(x == m)
                def _():
                    pltpu.make_async_copy(
                        YA.at[m, h], piece(out_ref, 0, h), o_recv.at[x, h]
                    ).start()

    for h in range(2):
        in_sent(h)
        out_all(h).wait_send()
        for sec in range(S):
            rows = out_ref.at[0, pl.ds(E * sec, E), pl.ds(h * LANES, LANES), :]
            pltpu.make_async_copy(rows, rows, o_recv.at[sec, h]).wait()
        for k in range(1, S):
            z_copy(k, h).wait_send()
            ya_copy(k, h).wait_send()
            o_copy(k, h).wait_send()

        @pl.when(x != m)
        def _():
            z_copy(0, h).wait_send()
            o_copy(0, h).wait_send()

    for turn, which in ((0, early), (1, late)):
        @pl.when(core == turn)
        def _():
            for i in which:
                for k in range(1, S):
                    w_copy(k, i).wait_send()
                    w_relay_copy(wrap(x + k, S), i).wait_send()


def per_device(pair_in, crop_mask, proj_weights, out_weights, up_weights, down_weights, norm_gains):
    S = lax.axis_size("section")
    G = lax.axis_size("axial") // S
    MB, R, N, C = pair_in.shape
    FF = up_weights.shape[-1]
    M = S * G
    MH = M // 2
    CPO = C // MH
    E = R // S
    assert G % 2 == 0
    assert MB == S and R == SUB and N == 2 * LANES and C == LANES and N == R * M
    any_spec = pl.BlockSpec(memory_space=pl.ANY)
    vmem_spec = pl.BlockSpec(memory_space=pltpu.VMEM)
    V = pltpu.VMEM
    dma = pltpu.SemaphoreType.DMA
    return pl.pallas_call(
        functools.partial(kernel, S, G, R, C, FF, S),
        out_shape=jax.ShapeDtypeStruct((1, R, N, C), BF16),
        in_specs=[any_spec, vmem_spec] + [any_spec] * 5,
        out_specs=any_spec,
        scratch_shapes=[
            V((2, R, LANES, C), BF16),
            V((2, R // 2, C, 2 * LANES), BF16),
            V((2, R // 2, C, 2 * LANES), BF16),
            V((2, R // 2, C, 2 * LANES), F32),
            V((2, MH, 2, CPO, SUB, LANES), BF16),
            V((2, 2, MH, CPO, SUB, LANES), BF16),
            V((2, 2, M, CPO, SUB, LANES), BF16),
            V((CPO, MH * SUB, 2 * LANES), F32),
            V((2, MH, CPO, SUB, LANES), BF16),
            V((2, MH, CPO, SUB, LANES), BF16),
            V((C * SUB, LANES), F32),
            V((C * SUB, LANES), F32),
            V((C * SUB, LANES), F32),
            V((SUB, LANES), F32),
            V((2, SUB, LANES), F32),
            V((2, R, LANES, C), BF16),
            V((S, 2, E, LANES, C), BF16),
            V((S, 5, C, C), BF16),
            V((S, C, C), BF16),
            V((S, C, FF), BF16),
            V((S, FF, C), BF16),
            V((S, 3, C), BF16),
            V((S, 5 * C, C), BF16),
            V((S, C, C), BF16),
            V((S, FF, C), BF16),
            V((S, C, FF), BF16),
            V((S, 3, C, LANES), F32),
        ]
        + [dma((2,))] * 5
        + [dma((2, 2))]
        + [dma((S, 2))] * 6
        + [dma((S, 5))] * 4,
        compiler_params=pltpu.CompilerParams(
            collective_id=0, has_side_effects=True, vmem_limit_bytes=56 * 1024 * 1024
        ),
    )(pair_in, crop_mask, proj_weights, out_weights, up_weights, down_weights, norm_gains)


def solution(mesh):
    return jax.shard_map(
        per_device,
        mesh=mesh,
        in_specs=(
            P("groups", "axial", None, None),
            P("groups", None),
            P("section", None, None, None),
            P("section", None, None),
            P("section", None, None),
            P("section", None, None),
            P("section", None, None),
        ),
        out_specs=P(("groups", "section"), "axial", None, None),
        check_vma=False,
    )
```

```python
import functools

import jax
import jax.numpy as jnp
from jax import lax
from jax.experimental import pallas as pl
from jax.experimental.pallas import tpu as pltpu
from jax.sharding import PartitionSpec as P

EPS = 1e-05
MESH = pl.DeviceIdType.MESH
F32 = jnp.float32
BF16 = jnp.bfloat16
LANES = 128
SUB = 8


def sigmoid(v):
    return 0.5 * jnp.tanh(0.5 * v) + 0.5


def norm_rows(v):
    center = v - jnp.mean(v, axis=0, keepdims=True)
    spread = jnp.mean(center * center, axis=0, keepdims=True)
    return center * lax.rsqrt(spread + EPS)


def mm(a, b):
    return jnp.dot(a, b, preferred_element_type=F32)


def kernel(
    S, G, R, C, FF, blocks,
    pair_ref, mask_ref, proj_ref, wout_ref, up_ref, down_ref, gain_ref,
    out_ref,
    ZIN, ZT, NB, GATE, SB, LL, RR, PART, TB, OB, S2L, S2R, S3, RS, PM, ZO, YA,
    WP, WO, WU, WD, GN, WPT, WOT, WUT, WDT, GC,
    l_send, l_recv, i_send, out_send, out_recv, i_recv,
    z_send, z_recv, ya_send, ya_recv, o_send, o_recv,
    w_send, w_recv, r_send, r_recv,
):
    M = S * G
    GH = G // 2
    MH = M // 2
    E = R // S
    CPO = C // MH
    x = lax.axis_index("section")
    A = lax.axis_index("axial")
    m = lax.div(A, G)
    t = lax.rem(A, G)
    a = x * G + t
    half = lax.div(t, GH)
    mine = x * GH + lax.rem(t, GH)

    def wrap(v, n):
        return lax.rem(v + 2 * n, n)

    def member(d):
        return {"section": lax.div(d, G), "axial": m * G + lax.rem(d, G)}

    def in_half(hf, i):
        return {"section": lax.div(i, GH), "axial": m * G + hf * GH + lax.rem(i, GH)}

    def along_x(sec):
        return {"section": sec, "axial": A}

    def remote(src, dst, ss, rs, dev):
        return pltpu.make_async_remote_copy(
            src_ref=src, dst_ref=dst, send_sem=ss, recv_sem=rs,
            device_id=dev, device_id_type=MESH,
        )

    barrier = pltpu.get_barrier_semaphore()

    def greet(k, c):
        pl.semaphore_signal(
            barrier, inc=1, device_id=member(lax.rem(a + k, M)), device_id_type=MESH
        )
        return c

    @pl.when(x != m)
    def _():
        for sec in range(S):
            pl.semaphore_signal(
                barrier, inc=1, device_id={"section": sec, "axial": x * G + t},
                device_id_type=MESH,
            )

    lax.fori_loop(1, M, greet, 0)
    pl.semaphore_wait(barrier, M - 1 + S - 1)

    def home(seg):
        return {"section": m, "axial": seg * G + t}

    def piece(ref, row, h):
        return ref.at[row, pl.ds(E * x, E), pl.ds(h * LANES, LANES), :]

    def z_copy(k, h):
        dest = wrap(m + k, S)
        return remote(
            piece(pair_ref, dest, h), ZIN.at[h, pl.ds(E * x, E)],
            z_send.at[k, h], z_recv.at[x, h], home(dest),
        )

    def z_start(k, h):
        if k:
            z_copy(k, h).start()
        else:
            @pl.when(x != m)
            def _():
                z_copy(0, h).start()

            @pl.when(x == m)
            def _():
                pltpu.make_async_copy(
                    piece(pair_ref, m, h), ZIN.at[h, pl.ds(E * x, E)], z_recv.at[x, h]
                ).start()

    weights = ((proj_ref, WP), (wout_ref, WO), (up_ref, WU), (down_ref, WD), (gain_ref, GN))

    def w_copy(k, i):
        src, dst = weights[i]
        return remote(
            src.at[0], dst.at[x], w_send.at[k, i], w_recv.at[k, i], along_x(wrap(x + k, S))
        )

    def w_local(i):
        src, dst = weights[i]
        return pltpu.make_async_copy(src.at[0], dst.at[x], w_recv.at[0, i])

    core = lax.rem(A, 2)
    sibling = A + 1 - 2 * core

    def w_relay_copy(l, i):
        dst = weights[i][1]
        return remote(
            dst.at[l], dst.at[l], r_send.at[l, i], r_recv.at[l, i],
            {"section": x, "axial": sibling},
        )

    def w_relay(l):
        k = wrap(x - l, S)
        for turn, which in ((0, early), (1, late)):
            @pl.when((x != l) & (core == turn))
            def _():
                for i in which:
                    dst = weights[i][1]
                    pltpu.make_async_copy(dst.at[l], dst.at[l], w_recv.at[k, i]).wait()
                    w_relay_copy(l, i).start()

    def w_arrived(l, which, turn):
        for i in which:
            dst = weights[i][1]

            @pl.when(x == l)
            def _():
                pltpu.make_async_copy(dst.at[l], dst.at[l], w_recv.at[0, i]).wait()

            @pl.when((x != l) & (core != turn))
            def _():
                w_relay_copy(l, i).wait_recv()

    early, late = (0, 4), (1, 2, 3)
    order = (S // 2,) + tuple(k for k in range(1, S) if k != S // 2)
    for h in range(2):
        for k in order + (0,):
            z_start(k, h)
    for i in early + late:
        w_local(i).start()
    for turn, which in ((0, early), (1, late)):
        @pl.when(core == turn)
        def _():
            for i in which:
                for k in order:
                    w_copy(k, i).start()

    q = mask_ref[pl.ds(m, 1), :].astype(F32)
    n_res = q.shape[1]
    lane = lax.broadcasted_iota(jnp.int32, (R, n_res), 1)
    row = lax.broadcasted_iota(jnp.int32, (R, n_res), 0) + a * R
    q_rows = jnp.sum(jnp.where(lane == row, q, 0.0), axis=1, keepdims=True)
    pair_mask = q_rows * q
    for h in range(2):
        PM[h] = pair_mask[:, h * LANES : (h + 1) * LANES]

    def flip(v):
        return v.astype(F32).T.astype(BF16)

    def flip_early(l):
        w_arrived(l, early, 0)
        for e in range(5):
            WPT[l, e * C : (e + 1) * C, :] = flip(WP[l, e])
        for g in range(3):
            GC[l, g] = jnp.broadcast_to(GN[l, g : g + 1, :].astype(F32), (LANES, C)).T

    def flip_late(l):
        w_arrived(l, late, 1)
        WOT[l] = flip(WO[l])
        for f in range(FF // C):
            WUT[l, f * C : (f + 1) * C, :] = flip(WU[l, :, f * C : (f + 1) * C])
            WDT[l, :, f * C : (f + 1) * C] = flip(WD[l, f * C : (f + 1) * C, :])

    def gather_in(h):
        for sec in range(S):
            rows = ZIN.at[h, pl.ds(E * sec, E)]
            pltpu.make_async_copy(rows, rows, z_recv.at[sec, h]).wait()

        for rp in range(R // 2):
            parts = [ZIN[h, 2 * rp + e].astype(F32).T for e in range(2)]
            turned = jnp.concatenate(parts, axis=1).astype(BF16)
            ZT[h, rp] = turned
            project(0, h, rp, turned.astype(F32))

        send_edges(0, h)

    def wide(v):
        return jnp.concatenate([v, v], axis=1)

    def left_copy(par, h, i):
        return remote(
            SB.at[h, i, 0], LL.at[par, h, mine], l_send.at[h], l_recv.at[h], in_half(half, i)
        )

    def right_copy(par, h, hf, i):
        return remote(
            SB.at[h, i, 1], RR.at[par, h, a], i_send.at[h], i_recv.at[par, h], in_half(hf, i)
        )

    def out_copy(h, i):
        return remote(
            TB.at[h, i], OB.at[h, mine], out_send.at[h], out_recv.at[h], in_half(half, i)
        )

    others = pl.ds(0, MH - 1)
    everyone = pl.ds(0, M - 1)

    def left_all(h):
        return remote(
            LL.at[0, h, others], LL.at[0, h, others], l_send.at[h], l_recv.at[h], member(lax.rem(a + 1, M))
        )

    def right_all(par, h):
        return remote(
            RR.at[par, h, everyone], RR.at[par, h, everyone],
            i_send.at[h], i_recv.at[par, h], member(lax.rem(a + 1, M)),
        )

    def out_all(h):
        return remote(
            TB.at[h, others], OB.at[h, others],
            out_send.at[h], out_recv.at[h], member(lax.rem(a + 1, M)),
        )

    def start_in(par, h):
        def go(k, c):
            i = lax.rem(mine + k, MH)
            j = lax.rem(mine + MH - k, MH)
            right_copy(par, h, 1 - half, i).start()

            @pl.when(k > 0)
            def _():
                left_copy(par, h, j).start()
                right_copy(par, h, half, j).start()

            return c

        lax.fori_loop(0, MH, go, 0)

    def start_out(h):
        def go(k, c):
            out_copy(h, lax.rem(mine + k, MH)).start()
            return c

        lax.fori_loop(1, MH, go, 0)

    def in_sent(h):
        left_all(h).wait_send()
        right_all(0, h).wait_send()

    def project(l, h, rp, z):
        normed = (norm_rows(z) * wide(GC[l, 0])).astype(BF16)
        NB[h, rp] = normed
        lin = mm(WPT[l, 0 : 4 * C, :], normed)
        pm = jnp.concatenate([PM[h, pl.ds(2 * rp + e, 1), :] for e in range(2)], axis=1)
        left = sigmoid(lin[C : 2 * C]) * lin[0:C] * pm
        right = sigmoid(lin[3 * C : 4 * C]) * lin[2 * C : 3 * C] * pm
        for e in range(2):
            rows = pl.ds(2 * rp + e, C, stride=SUB)
            S2L[rows, :] = left[:, e * LANES : (e + 1) * LANES]
            S2R[rows, :] = right[:, e * LANES : (e + 1) * LANES]

    def send_edges(l, h):
        @pl.when(l > 0)
        def _():
            in_sent(h)

        par = l % 2
        SB[h, :, 0] = S2L[...].reshape(MH, CPO, SUB, LANES).astype(BF16)
        SB[h, :, 1] = S2R[...].reshape(MH, CPO, SUB, LANES).astype(BF16)
        start_in(par, h)
        LL[par, h, mine] = SB[h, mine, 0]
        RR[par, h, a] = SB[h, mine, 1]

        def gates(rp, c):
            GATE[h, rp] = sigmoid(mm(WPT[l, 4 * C : 5 * C, :], NB[h, rp]))
            return c

        [gates(rp, 0) for rp in range(R // 2)]

    def triangle(l):
        par = l % 2

        def flat(v):
            return v.astype(F32).reshape(-1, LANES).astype(BF16)

        def outer(p, q):
            return lax.dot_general(
                flat(p), flat(q), (((1,), (1,)), ((), ())), preferred_element_type=F32
            )

        def arrived(e):
            left_all(e).wait_recv()
            right_all(par, e).wait_recv()

        def first(c, carry):
            PART[c] = outer(LL[par, 0, :, c], RR[par, 0, :, c])
            return carry

        arrived(0)
        lax.fori_loop(0, CPO, first, 0, unroll=2)

        @pl.when(l > 0)
        def _():
            for h in range(2):
                out_all(h).wait_send()

        arrived(1)
        for h in range(2):
            def channel(c, carry):
                prod = PART[c, :, h * LANES : (h + 1) * LANES] + outer(
                    LL[par, 1, :, c], RR[par, 1, h * MH : (h + 1) * MH, c]
                )
                TB[h, :, c] = prod.reshape(MH, SUB, LANES).astype(BF16)
                return carry

            lax.fori_loop(0, CPO, channel, 0, unroll=True)
            start_out(h)
            OB[h, mine] = TB[h, mine]

    def post(l, h, follow):
        out_all(h).wait_recv()
        got = OB[h].astype(F32).reshape(C, SUB, LANES)
        mean = jnp.sum(got, axis=0) * (1.0 / C)
        center = got - mean[None]
        S3[...] = center.reshape(C * SUB, LANES)
        RS[...] = lax.rsqrt(jnp.sum(center * center, axis=0) * (1.0 / C) + EPS)
        g1 = wide(GC[l, 1])
        g2 = wide(GC[l, 2])

        for rp in range(R // 2):
            vals = jnp.concatenate(
                [S3[pl.ds(2 * rp + e, C, stride=SUB), :] for e in range(2)], axis=1
            )
            scale = jnp.concatenate([RS[pl.ds(2 * rp + e, 1), :] for e in range(2)], axis=1)
            tri_norm = (vals * scale * g1).astype(BF16)
            mid = ZT[h, rp].astype(F32) + GATE[h, rp] * mm(WOT[l], tri_norm)
            trans_in = (norm_rows(mid) * g2).astype(BF16)
            hidden = jnp.maximum(mm(WUT[l], trans_in), 0.0).astype(BF16)
            new = (mid + mm(WDT[l], hidden)).astype(BF16)
            ZT[h, rp] = new
            if follow:
                project(l + 1, h, rp, new.astype(F32))


    def ya_copy(k, h):
        sec = wrap(x + k, S)
        return remote(
            ZO.at[h, pl.ds(E * sec, E)], YA.at[x, h],
            ya_send.at[k, h], ya_recv.at[k, h], along_x(sec),
        )

    def o_copy(k, h):
        seg = wrap(m + k, S)
        return remote(
            YA.at[seg, h], piece(out_ref, 0, h), o_send.at[k, h], o_recv.at[x, h], home(seg)
        )

    def spread(h):
        for rp in range(R // 2):
            v = ZT[h, rp].astype(F32)
            for e in range(2):
                ZO[h, 2 * rp + e] = v[:, e * LANES : (e + 1) * LANES].T.astype(BF16)
        for k in order:
            ya_copy(k, h).start()
        YA[x, h] = ZO[h, pl.ds(E * x, E)]

    w_relay(0)
    flip_early(0)
    gather_in(0)
    for l in range(1, blocks):
        w_relay(l)
    gather_in(1)

    def block(l, c):
        flip_late(l)
        flip_early(l + 1)
        triangle(l)
        for h in range(2):
            post(l, h, True)
            send_edges(l + 1, h)
        return c

    lax.fori_loop(0, blocks - 1, block, 0)
    flip_late(blocks - 1)
    triangle(blocks - 1)
    for h in range(2):
        post(blocks - 1, h, False)
        spread(h)

    for h in range(2):
        for k in order + (0,):
            seg = wrap(m + k, S)
            kx = wrap(x - seg, S)

            @pl.when(kx != 0)
            def _():
                pltpu.make_async_copy(YA.at[seg, h], YA.at[seg, h], ya_recv.at[kx, h]).wait()

            if k:
                o_copy(k, h).start()
            else:
                @pl.when(x != m)
                def _():
                    o_copy(0, h).start()

                @pl.when(x == m)
                def _():
                    pltpu.make_async_copy(
                        YA.at[m, h], piece(out_ref, 0, h), o_recv.at[x, h]
                    ).start()

    for h in range(2):
        in_sent(h)
        out_all(h).wait_send()
        for sec in range(S):
            rows = out_ref.at[0, pl.ds(E * sec, E), pl.ds(h * LANES, LANES), :]
            pltpu.make_async_copy(rows, rows, o_recv.at[sec, h]).wait()
        for k in range(1, S):
            z_copy(k, h).wait_send()
            ya_copy(k, h).wait_send()
            o_copy(k, h).wait_send()

        @pl.when(x != m)
        def _():
            z_copy(0, h).wait_send()
            o_copy(0, h).wait_send()

    for turn, which in ((0, early), (1, late)):
        @pl.when(core == turn)
        def _():
            for i in which:
                for k in range(1, S):
                    w_copy(k, i).wait_send()
                    w_relay_copy(wrap(x + k, S), i).wait_send()


def per_device(pair_in, crop_mask, proj_weights, out_weights, up_weights, down_weights, norm_gains):
    S = lax.axis_size("section")
    G = lax.axis_size("axial") // S
    MB, R, N, C = pair_in.shape
    FF = up_weights.shape[-1]
    M = S * G
    MH = M // 2
    CPO = C // MH
    E = R // S
    assert G % 2 == 0
    assert MB == S and R == SUB and N == 2 * LANES and C == LANES and N == R * M
    any_spec = pl.BlockSpec(memory_space=pl.ANY)
    vmem_spec = pl.BlockSpec(memory_space=pltpu.VMEM)
    V = pltpu.VMEM
    dma = pltpu.SemaphoreType.DMA
    return pl.pallas_call(
        functools.partial(kernel, S, G, R, C, FF, S),
        out_shape=jax.ShapeDtypeStruct((1, R, N, C), BF16),
        in_specs=[any_spec, vmem_spec] + [any_spec] * 5,
        out_specs=any_spec,
        scratch_shapes=[
            V((2, R, LANES, C), BF16),
            V((2, R // 2, C, 2 * LANES), BF16),
            V((2, R // 2, C, 2 * LANES), BF16),
            V((2, R // 2, C, 2 * LANES), F32),
            V((2, MH, 2, CPO, SUB, LANES), BF16),
            V((2, 2, MH, CPO, SUB, LANES), BF16),
            V((2, 2, M, CPO, SUB, LANES), BF16),
            V((CPO, MH * SUB, 2 * LANES), F32),
            V((2, MH, CPO, SUB, LANES), BF16),
            V((2, MH, CPO, SUB, LANES), BF16),
            V((C * SUB, LANES), F32),
            V((C * SUB, LANES), F32),
            V((C * SUB, LANES), F32),
            V((SUB, LANES), F32),
            V((2, SUB, LANES), F32),
            V((2, R, LANES, C), BF16),
            V((S, 2, E, LANES, C), BF16),
            V((S, 5, C, C), BF16),
            V((S, C, C), BF16),
            V((S, C, FF), BF16),
            V((S, FF, C), BF16),
            V((S, 3, C), BF16),
            V((S, 5 * C, C), BF16),
            V((S, C, C), BF16),
            V((S, FF, C), BF16),
            V((S, C, FF), BF16),
            V((S, 3, C, LANES), F32),
        ]
        + [dma((2,))] * 5
        + [dma((2, 2))]
        + [dma((S, 2))] * 6
        + [dma((S, 5))] * 4,
        compiler_params=pltpu.CompilerParams(
            collective_id=0, has_side_effects=True, vmem_limit_bytes=56 * 1024 * 1024
        ),
    )(pair_in, crop_mask, proj_weights, out_weights, up_weights, down_weights, norm_gains)


def solution(mesh):
    return jax.shard_map(
        per_device,
        mesh=mesh,
        in_specs=(
            P("groups", "axial", None, None),
            P("groups", None),
            P("section", None, None, None),
            P("section", None, None),
            P("section", None, None),
            P("section", None, None),
            P("section", None, None),
        ),
        out_specs=P(("groups", "section"), "axial", None, None),
        check_vma=False,
    )
```

```python
import functools

import jax
import jax.numpy as jnp
from jax import lax
from jax.experimental import pallas as pl
from jax.experimental.pallas import tpu as pltpu
from jax.sharding import PartitionSpec as P

EPS = 1e-05
MESH = pl.DeviceIdType.MESH
F32 = jnp.float32
BF16 = jnp.bfloat16
LANES = 128
SUB = 8


def sigmoid(v):
    return 0.5 * jnp.tanh(0.5 * v) + 0.5


def norm_rows(v):
    center = v - jnp.mean(v, axis=0, keepdims=True)
    spread = jnp.mean(center * center, axis=0, keepdims=True)
    return center * lax.rsqrt(spread + EPS)


def mm(a, b):
    return jnp.dot(a, b, preferred_element_type=F32)


def kernel(
    S, G, R, C, FF, blocks,
    pair_ref, mask_ref, proj_ref, wout_ref, up_ref, down_ref, gain_ref,
    out_ref,
    ZIN, ZT, NB, GATE, SB, LL, RR, PART, TB, OB, S2L, S2R, S3, RS, PM, ZO, YA,
    WP, WO, WU, WD, GN, WPT, WOT, WUT, WDT, GC,
    l_send, l_recv, i_send, out_send, out_recv, i_recv,
    z_send, z_recv, ya_send, ya_recv, o_send, o_recv,
    w_send, w_recv, r_send, r_recv,
):
    M = S * G
    GH = G // 2
    MH = M // 2
    E = R // S
    CPO = C // MH
    x = lax.axis_index("section")
    A = lax.axis_index("axial")
    m = lax.div(A, G)
    t = lax.rem(A, G)
    a = x * G + t
    half = lax.div(t, GH)
    mine = x * GH + lax.rem(t, GH)

    def wrap(v, n):
        return lax.rem(v + 2 * n, n)

    def member(d):
        return {"section": lax.div(d, G), "axial": m * G + lax.rem(d, G)}

    def in_half(hf, i):
        return {"section": lax.div(i, GH), "axial": m * G + hf * GH + lax.rem(i, GH)}

    def along_x(sec):
        return {"section": sec, "axial": A}

    def remote(src, dst, ss, rs, dev):
        return pltpu.make_async_remote_copy(
            src_ref=src, dst_ref=dst, send_sem=ss, recv_sem=rs,
            device_id=dev, device_id_type=MESH,
        )

    barrier = pltpu.get_barrier_semaphore()

    def greet(k, c):
        pl.semaphore_signal(
            barrier, inc=1, device_id=member(lax.rem(a + k, M)), device_id_type=MESH
        )
        return c

    @pl.when(x != m)
    def _():
        for sec in range(S):
            pl.semaphore_signal(
                barrier, inc=1, device_id={"section": sec, "axial": x * G + t},
                device_id_type=MESH,
            )

    lax.fori_loop(1, M, greet, 0)
    pl.semaphore_wait(barrier, M - 1 + S - 1)

    def home(seg):
        return {"section": m, "axial": seg * G + t}

    def piece(ref, row, h):
        return ref.at[row, pl.ds(E * x, E), pl.ds(h * LANES, LANES), :]

    def z_copy(k, h):
        dest = wrap(m + k, S)
        return remote(
            piece(pair_ref, dest, h), ZIN.at[h, pl.ds(E * x, E)],
            z_send.at[k, h], z_recv.at[x, h], home(dest),
        )

    def z_start(k, h):
        if k:
            z_copy(k, h).start()
        else:
            @pl.when(x != m)
            def _():
                z_copy(0, h).start()

            @pl.when(x == m)
            def _():
                pltpu.make_async_copy(
                    piece(pair_ref, m, h), ZIN.at[h, pl.ds(E * x, E)], z_recv.at[x, h]
                ).start()

    weights = ((proj_ref, WP), (wout_ref, WO), (up_ref, WU), (down_ref, WD), (gain_ref, GN))

    def w_copy(k, i):
        src, dst = weights[i]
        return remote(
            src.at[0], dst.at[x], w_send.at[k, i], w_recv.at[k, i], along_x(wrap(x + k, S))
        )

    def w_local(i):
        src, dst = weights[i]
        return pltpu.make_async_copy(src.at[0], dst.at[x], w_recv.at[0, i])

    core = lax.rem(A, 2)
    sibling = A + 1 - 2 * core

    def w_relay_copy(l, i):
        dst = weights[i][1]
        return remote(
            dst.at[l], dst.at[l], r_send.at[l, i], r_recv.at[l, i],
            {"section": x, "axial": sibling},
        )

    def w_relay(l):
        k = wrap(x - l, S)
        for turn, which in ((0, early), (1, late)):
            @pl.when((x != l) & (core == turn))
            def _():
                for i in which:
                    dst = weights[i][1]
                    pltpu.make_async_copy(dst.at[l], dst.at[l], w_recv.at[k, i]).wait()
                    w_relay_copy(l, i).start()

    def w_arrived(l, which, turn):
        for i in which:
            dst = weights[i][1]

            @pl.when(x == l)
            def _():
                pltpu.make_async_copy(dst.at[l], dst.at[l], w_recv.at[0, i]).wait()

            @pl.when((x != l) & (core != turn))
            def _():
                w_relay_copy(l, i).wait_recv()

    early, late = (0, 4), (1, 2, 3)
    order = (S // 2,) + tuple(k for k in range(1, S) if k != S // 2)
    for h in range(2):
        for k in order + (0,):
            z_start(k, h)
    for i in early + late:
        w_local(i).start()
    for turn, which in ((0, early), (1, late)):
        @pl.when(core == turn)
        def _():
            for i in which:
                for k in order:
                    w_copy(k, i).start()

    q = mask_ref[pl.ds(m, 1), :].astype(F32)
    n_res = q.shape[1]
    lane = lax.broadcasted_iota(jnp.int32, (R, n_res), 1)
    row = lax.broadcasted_iota(jnp.int32, (R, n_res), 0) + a * R
    q_rows = jnp.sum(jnp.where(lane == row, q, 0.0), axis=1, keepdims=True)
    pair_mask = q_rows * q
    for h in range(2):
        PM[h] = pair_mask[:, h * LANES : (h + 1) * LANES]

    def flip(v):
        return v.astype(F32).T.astype(BF16)

    def flip_early(l):
        w_arrived(l, early, 0)
        for e in range(5):
            WPT[l, e * C : (e + 1) * C, :] = flip(WP[l, e])
        for g in range(3):
            GC[l, g] = jnp.broadcast_to(GN[l, g : g + 1, :].astype(F32), (LANES, C)).T

    def flip_late(l):
        w_arrived(l, late, 1)
        WOT[l] = flip(WO[l])
        for f in range(FF // C):
            WUT[l, f * C : (f + 1) * C, :] = flip(WU[l, :, f * C : (f + 1) * C])
            WDT[l, :, f * C : (f + 1) * C] = flip(WD[l, f * C : (f + 1) * C, :])

    def gather_in(h):
        for sec in range(S):
            rows = ZIN.at[h, pl.ds(E * sec, E)]
            pltpu.make_async_copy(rows, rows, z_recv.at[sec, h]).wait()

        for rp in range(R // 2):
            parts = [ZIN[h, 2 * rp + e].astype(F32).T for e in range(2)]
            turned = jnp.concatenate(parts, axis=1).astype(BF16)
            ZT[h, rp] = turned
            project(0, h, rp, turned.astype(F32))

        send_edges(0, h)

    def wide(v):
        return jnp.concatenate([v, v], axis=1)

    def left_copy(par, h, i):
        return remote(
            SB.at[h, i, 0], LL.at[par, h, mine], l_send.at[h], l_recv.at[h], in_half(half, i)
        )

    def right_copy(par, h, hf, i):
        return remote(
            SB.at[h, i, 1], RR.at[par, h, a], i_send.at[h], i_recv.at[par, h], in_half(hf, i)
        )

    def out_copy(h, i):
        return remote(
            TB.at[h, i], OB.at[h, mine], out_send.at[h], out_recv.at[h], in_half(half, i)
        )

    others = pl.ds(0, MH - 1)
    everyone = pl.ds(0, M - 1)

    def left_all(h):
        return remote(
            LL.at[0, h, others], LL.at[0, h, others], l_send.at[h], l_recv.at[h], member(lax.rem(a + 1, M))
        )

    def right_all(par, h):
        return remote(
            RR.at[par, h, everyone], RR.at[par, h, everyone],
            i_send.at[h], i_recv.at[par, h], member(lax.rem(a + 1, M)),
        )

    def out_all(h):
        return remote(
            TB.at[h, others], OB.at[h, others],
            out_send.at[h], out_recv.at[h], member(lax.rem(a + 1, M)),
        )

    def start_in(par, h):
        def go(k, c):
            i = lax.rem(mine + k, MH)
            j = lax.rem(mine + MH - k, MH)
            right_copy(par, h, 1 - half, i).start()

            @pl.when(k > 0)
            def _():
                left_copy(par, h, j).start()
                right_copy(par, h, half, j).start()

            return c

        lax.fori_loop(0, MH, go, 0)

    def start_out(h):
        def go(k, c):
            out_copy(h, lax.rem(mine + k, MH)).start()
            return c

        lax.fori_loop(1, MH, go, 0)

    def in_sent(h):
        left_all(h).wait_send()
        right_all(0, h).wait_send()

    def project(l, h, rp, z):
        normed = (norm_rows(z) * wide(GC[l, 0])).astype(BF16)
        NB[h, rp] = normed
        lin = mm(WPT[l, 0 : 4 * C, :], normed)
        pm = jnp.concatenate([PM[h, pl.ds(2 * rp + e, 1), :] for e in range(2)], axis=1)
        left = sigmoid(lin[C : 2 * C]) * lin[0:C] * pm
        right = sigmoid(lin[3 * C : 4 * C]) * lin[2 * C : 3 * C] * pm
        for e in range(2):
            rows = pl.ds(2 * rp + e, C, stride=SUB)
            S2L[rows, :] = left[:, e * LANES : (e + 1) * LANES]
            S2R[rows, :] = right[:, e * LANES : (e + 1) * LANES]

    def send_edges(l, h):
        @pl.when(l > 0)
        def _():
            in_sent(h)

        par = l % 2
        SB[h, :, 0] = S2L[...].reshape(MH, CPO, SUB, LANES).astype(BF16)
        SB[h, :, 1] = S2R[...].reshape(MH, CPO, SUB, LANES).astype(BF16)
        start_in(par, h)
        LL[par, h, mine] = SB[h, mine, 0]
        RR[par, h, a] = SB[h, mine, 1]

        def gates(rp, c):
            GATE[h, rp] = sigmoid(mm(WPT[l, 4 * C : 5 * C, :], NB[h, rp]))
            return c

        [gates(rp, 0) for rp in range(R // 2)]

    def triangle(l):
        par = l % 2

        def flat(v):
            return v.astype(F32).reshape(-1, LANES).astype(BF16)

        def outer(p, q):
            return lax.dot_general(
                flat(p), flat(q), (((1,), (1,)), ((), ())), preferred_element_type=F32
            )

        def arrived(e):
            left_all(e).wait_recv()
            right_all(par, e).wait_recv()

        def first(c, carry):
            PART[c] = outer(LL[par, 0, :, c], RR[par, 0, :, c])
            return carry

        arrived(0)
        lax.fori_loop(0, CPO, first, 0, unroll=2)

        @pl.when(l > 0)
        def _():
            for h in range(2):
                out_all(h).wait_send()

        arrived(1)
        for h in range(2):
            def channel(c, carry):
                prod = PART[c, :, h * LANES : (h + 1) * LANES] + outer(
                    LL[par, 1, :, c], RR[par, 1, h * MH : (h + 1) * MH, c]
                )
                TB[h, :, c] = prod.reshape(MH, SUB, LANES).astype(BF16)
                return carry

            lax.fori_loop(0, CPO, channel, 0, unroll=True)
            start_out(h)
            OB[h, mine] = TB[h, mine]

    def post(l, h, follow):
        out_all(h).wait_recv()
        got = OB[h].astype(F32).reshape(C, SUB, LANES)
        mean = jnp.sum(got, axis=0) * (1.0 / C)
        center = got - mean[None]
        S3[...] = center.reshape(C * SUB, LANES)
        RS[...] = lax.rsqrt(jnp.sum(center * center, axis=0) * (1.0 / C) + EPS)
        g1 = wide(GC[l, 1])
        g2 = wide(GC[l, 2])

        for rp in range(R // 2):
            vals = jnp.concatenate(
                [S3[pl.ds(2 * rp + e, C, stride=SUB), :] for e in range(2)], axis=1
            )
            scale = jnp.concatenate([RS[pl.ds(2 * rp + e, 1), :] for e in range(2)], axis=1)
            tri_norm = (vals * scale * g1).astype(BF16)
            mid = ZT[h, rp].astype(F32) + GATE[h, rp] * mm(WOT[l], tri_norm)
            trans_in = (norm_rows(mid) * g2).astype(BF16)
            hidden = jnp.maximum(mm(WUT[l], trans_in), 0.0).astype(BF16)
            new = (mid + mm(WDT[l], hidden)).astype(BF16)
            ZT[h, rp] = new
            if follow:
                project(l + 1, h, rp, new.astype(F32))


    def ya_copy(k, h):
        sec = wrap(x + k, S)
        return remote(
            ZO.at[h, pl.ds(E * sec, E)], YA.at[x, h],
            ya_send.at[k, h], ya_recv.at[k, h], along_x(sec),
        )

    def o_copy(k, h):
        seg = wrap(m + k, S)
        return remote(
            YA.at[seg, h], piece(out_ref, 0, h), o_send.at[k, h], o_recv.at[x, h], home(seg)
        )

    def spread(h):
        for rp in range(R // 2):
            v = ZT[h, rp].astype(F32)
            for e in range(2):
                ZO[h, 2 * rp + e] = v[:, e * LANES : (e + 1) * LANES].T.astype(BF16)
        for k in order:
            ya_copy(k, h).start()
        YA[x, h] = ZO[h, pl.ds(E * x, E)]

    def place(h):
        for k in order + (0,):
            seg = wrap(m + k, S)
            kx = wrap(x - seg, S)

            @pl.when(kx != 0)
            def _():
                pltpu.make_async_copy(YA.at[seg, h], YA.at[seg, h], ya_recv.at[kx, h]).wait()

            if k:
                o_copy(k, h).start()
            else:
                @pl.when(x != m)
                def _():
                    o_copy(0, h).start()

                @pl.when(x == m)
                def _():
                    pltpu.make_async_copy(
                        YA.at[m, h], piece(out_ref, 0, h), o_recv.at[x, h]
                    ).start()

    w_relay(0)
    flip_early(0)
    gather_in(0)
    for l in range(1, blocks):
        w_relay(l)
    gather_in(1)

    def block(l, c):
        flip_late(l)
        flip_early(l + 1)
        triangle(l)
        for h in range(2):
            post(l, h, True)
            send_edges(l + 1, h)
        return c

    lax.fori_loop(0, blocks - 1, block, 0)
    flip_late(blocks - 1)
    triangle(blocks - 1)
    post(blocks - 1, 0, False)
    spread(0)
    post(blocks - 1, 1, False)
    place(0)
    spread(1)
    place(1)

    for h in range(2):
        in_sent(h)
        out_all(h).wait_send()
        for sec in range(S):
            rows = out_ref.at[0, pl.ds(E * sec, E), pl.ds(h * LANES, LANES), :]
            pltpu.make_async_copy(rows, rows, o_recv.at[sec, h]).wait()
        for k in range(1, S):
            z_copy(k, h).wait_send()
            ya_copy(k, h).wait_send()
            o_copy(k, h).wait_send()

        @pl.when(x != m)
        def _():
            z_copy(0, h).wait_send()
            o_copy(0, h).wait_send()

    for turn, which in ((0, early), (1, late)):
        @pl.when(core == turn)
        def _():
            for i in which:
                for k in range(1, S):
                    w_copy(k, i).wait_send()
                    w_relay_copy(wrap(x + k, S), i).wait_send()


def per_device(pair_in, crop_mask, proj_weights, out_weights, up_weights, down_weights, norm_gains):
    S = lax.axis_size("section")
    G = lax.axis_size("axial") // S
    MB, R, N, C = pair_in.shape
    FF = up_weights.shape[-1]
    M = S * G
    MH = M // 2
    CPO = C // MH
    E = R // S
    assert G % 2 == 0
    assert MB == S and R == SUB and N == 2 * LANES and C == LANES and N == R * M
    any_spec = pl.BlockSpec(memory_space=pl.ANY)
    vmem_spec = pl.BlockSpec(memory_space=pltpu.VMEM)
    V = pltpu.VMEM
    dma = pltpu.SemaphoreType.DMA
    return pl.pallas_call(
        functools.partial(kernel, S, G, R, C, FF, S),
        out_shape=jax.ShapeDtypeStruct((1, R, N, C), BF16),
        in_specs=[any_spec, vmem_spec] + [any_spec] * 5,
        out_specs=any_spec,
        scratch_shapes=[
            V((2, R, LANES, C), BF16),
            V((2, R // 2, C, 2 * LANES), BF16),
            V((2, R // 2, C, 2 * LANES), BF16),
            V((2, R // 2, C, 2 * LANES), F32),
            V((2, MH, 2, CPO, SUB, LANES), BF16),
            V((2, 2, MH, CPO, SUB, LANES), BF16),
            V((2, 2, M, CPO, SUB, LANES), BF16),
            V((CPO, MH * SUB, 2 * LANES), F32),
            V((2, MH, CPO, SUB, LANES), BF16),
            V((2, MH, CPO, SUB, LANES), BF16),
            V((C * SUB, LANES), F32),
            V((C * SUB, LANES), F32),
            V((C * SUB, LANES), F32),
            V((SUB, LANES), F32),
            V((2, SUB, LANES), F32),
            V((2, R, LANES, C), BF16),
            V((S, 2, E, LANES, C), BF16),
            V((S, 5, C, C), BF16),
            V((S, C, C), BF16),
            V((S, C, FF), BF16),
            V((S, FF, C), BF16),
            V((S, 3, C), BF16),
            V((S, 5 * C, C), BF16),
            V((S, C, C), BF16),
            V((S, FF, C), BF16),
            V((S, C, FF), BF16),
            V((S, 3, C, LANES), F32),
        ]
        + [dma((2,))] * 5
        + [dma((2, 2))]
        + [dma((S, 2))] * 6
        + [dma((S, 5))] * 4,
        compiler_params=pltpu.CompilerParams(
            collective_id=0, has_side_effects=True, vmem_limit_bytes=56 * 1024 * 1024
        ),
    )(pair_in, crop_mask, proj_weights, out_weights, up_weights, down_weights, norm_gains)


def solution(mesh):
    return jax.shard_map(
        per_device,
        mesh=mesh,
        in_specs=(
            P("groups", "axial", None, None),
            P("groups", None),
            P("section", None, None, None),
            P("section", None, None),
            P("section", None, None),
            P("section", None, None),
            P("section", None, None),
        ),
        out_specs=P(("groups", "section"), "axial", None, None),
        check_vma=False,
    )
```
